64 devices in a mesh: dp: 4 (over x, y), kv: 16 (over z, core).
Axes of the slice: x: 2, y: 2, z: 8, core: 2. Of those that a mesh axis runs over, the one named last changes fastest.
The devices are a block of a 4x4x8 slice.
Arguments:
- x_first: bfloat16 [64, 4096], P('dp'), parts along dimension 0
- next_emb: bfloat16 [2, 64, 4096], P(None, 'dp'), parts along dimension 1
- k_cache: bfloat16 [64, 4096, 4, 128], P('dp', 'kv'), parts along dimension 0
- v_cache: bfloat16 [64, 4096, 4, 128], P('dp', 'kv'), parts along dimension 0
- seq_len: int32 [64], P('dp'), parts along dimension 0
- ln1_gain: float32 [4096], replicated
- ln1_bias: float32 [4096], replicated
- w_q: bfloat16 [4096, 2048], replicated
- b_q: float32 [2048], replicated
- w_k: bfloat16 [4096, 512], replicated
- b_k: float32 [512], replicated
- w_v: bfloat16 [4096, 512], replicated
- b_v: float32 [512], replicated
- w_o: bfloat16 [2048, 4096], replicated
- b_o: float32 [4096], replicated
- ln2_gain: float32 [4096], replicated
- ln2_bias: float32 [4096], replicated
- w_router: bfloat16 [4096, 16], replicated
- w_gate: bfloat16 [16, 4096, 448], P(None, None, 'kv')
- w_up: bfloat16 [16, 4096, 448], P(None, None, 'kv')
- w_down: bfloat16 [16, 448, 4096], P(None, 'kv')
- long_factor: float32 [64], replicated
- expert_idx: int32 [3, 64, 2], P(None, 'dp'), parts along dimension 1
- route_mask: int32 [3, 64, 2, 16], P(None, 'dp'), parts along dimension 1
Outputs:
- output 1: bfloat16 [3, 64, 4096], P(None, 'dp'), parts along dimension 1
- output 2: bfloat16 [64, 3, 4, 128], P('dp'), parts along dimension 0
- output 3: bfloat16 [64, 3, 4, 128], P('dp'), parts along dimension 0
There are 4 independent parts. The reference program is written for one: setup_inputs(seed, part) draws one part's arguments, and reference() takes and returns one part's arrays. A program takes and returns all parts, laid end to end along the dimension named above; an argument that names none is the same for every part.
All inputs are finite; a program needn't handle non-finite values.
Results may differ from the reference program's by a relative error of at most 0.0117778.
Values sent between devices are 32-bit elements.
A program may use at most 768 MiB of HBM per device.

```python
import math
import jax
import jax.numpy as jnp
from jax import lax

BATCH_SIZE = 16
SHARD_LEN = 256
KV_GROUP = 16
CACHE_LEN = 4096
D_MODEL = 4096
Q_HEADS = 16
KV_HEADS = 4
HEAD_DIM = 128
NUM_EXPERTS = 16
TOP_K = 2
FF_DIM = 448
NUM_STEPS = 3
SEG_COUNT = 64

HALF_DIM = HEAD_DIM // 2
Q_GROUP = Q_HEADS // KV_HEADS
FF_SHARD = FF_DIM // KV_GROUP
ROPE_BASE = 10000.0
ROPE_MSCALE = math.sqrt(1.0 + math.log(32.0) / math.log(4096.0))
NORM_EPS = 1e-5
NEG_FILL = -1e30


def setup_inputs(seed: int = 0, part: int = 0) -> dict:
    base_key = jax.random.key(seed)
    shared_keys = jax.random.split(base_key, 17)
    part_keys = jax.random.split(jax.random.fold_in(base_key, part), 9)
    q_width = Q_HEADS * HEAD_DIM
    kv_width = KV_HEADS * HEAD_DIM
    d_scale = D_MODEL ** -0.5

    def normal(rand_key, arr_dims, factor):
        return jax.random.normal(rand_key, arr_dims, jnp.float32) * factor

    x_first = normal(part_keys[0], (BATCH_SIZE, D_MODEL), 1.0).astype(jnp.bfloat16)
    next_emb = normal(part_keys[1], (NUM_STEPS - 1, BATCH_SIZE, D_MODEL), 1.0).astype(jnp.bfloat16)
    seg_index = (jnp.arange(CACHE_LEN) * SEG_COUNT) // CACHE_LEN
    key_segs = normal(part_keys[2], (BATCH_SIZE, SEG_COUNT, KV_HEADS, HEAD_DIM), 1.0)
    value_segs = normal(part_keys[3], (BATCH_SIZE, SEG_COUNT, KV_HEADS, HEAD_DIM), 4.0)
    cache_dims = (BATCH_SIZE, CACHE_LEN, KV_HEADS, HEAD_DIM)
    k_cache = (normal(part_keys[4], cache_dims, 1.0) + key_segs[:, seg_index]).astype(jnp.bfloat16)
    v_cache = (normal(part_keys[5], cache_dims, 1.0) + value_segs[:, seg_index]).astype(jnp.bfloat16)
    drawn_lens = jax.random.randint(part_keys[6], (BATCH_SIZE,), CACHE_LEN // 4, CACHE_LEN + 1)
    seq_len = jnp.where(jnp.arange(BATCH_SIZE) == 0, CACHE_LEN, drawn_lens).astype(jnp.int32)
    rank_scores = jax.random.randint(part_keys[7], (NUM_STEPS, BATCH_SIZE, NUM_EXPERTS), 0, 1 << 20)
    expert_order = jnp.argsort(rank_scores * NUM_EXPERTS + jnp.arange(NUM_EXPERTS), axis=-1)
    expert_idx = expert_order[..., :TOP_K].astype(jnp.int32)
    chosen = (expert_idx[..., None] == jnp.arange(NUM_EXPERTS)).astype(jnp.int32)
    earlier = jnp.cumsum(chosen, axis=2) - chosen
    coin_flip = jax.random.randint(part_keys[8], (NUM_STEPS, BATCH_SIZE, TOP_K, NUM_EXPERTS), 0, 2)
    route_mask = jnp.where(chosen == 1, 1, jnp.where(earlier > 0, 0, coin_flip)).astype(jnp.int32)
    return {
        'x_first': x_first,
        'next_emb': next_emb,
        'k_cache': k_cache,
        'v_cache': v_cache,
        'seq_len': seq_len,
        'ln1_gain': 1.0 + normal(shared_keys[0], (D_MODEL,), 0.3),
        'ln1_bias': normal(shared_keys[1], (D_MODEL,), 0.3),
        'w_q': normal(shared_keys[2], (D_MODEL, q_width), d_scale).astype(jnp.bfloat16),
        'b_q': normal(shared_keys[3], (q_width,), 0.5),
        'w_k': normal(shared_keys[4], (D_MODEL, kv_width), d_scale).astype(jnp.bfloat16),
        'b_k': normal(shared_keys[5], (kv_width,), 0.5),
        'w_v': normal(shared_keys[6], (D_MODEL, kv_width), d_scale).astype(jnp.bfloat16),
        'b_v': normal(shared_keys[7], (kv_width,), 0.5),
        'w_o': normal(shared_keys[8], (q_width, D_MODEL), q_width ** -0.5).astype(jnp.bfloat16),
        'b_o': normal(shared_keys[9], (D_MODEL,), 0.3),
        'ln2_gain': 1.0 + normal(shared_keys[10], (D_MODEL,), 0.3),
        'ln2_bias': normal(shared_keys[11], (D_MODEL,), 0.3),
        'w_router': normal(shared_keys[12], (D_MODEL, NUM_EXPERTS), 1.5 * d_scale).astype(jnp.bfloat16),
        'w_gate': normal(shared_keys[13], (NUM_EXPERTS, D_MODEL, FF_DIM), d_scale).astype(jnp.bfloat16),
        'w_up': normal(shared_keys[14], (NUM_EXPERTS, D_MODEL, FF_DIM), d_scale).astype(jnp.bfloat16),
        'w_down': normal(shared_keys[15], (NUM_EXPERTS, FF_DIM, D_MODEL), FF_DIM ** -0.5).astype(jnp.bfloat16),
        'long_factor': jnp.exp(jax.random.uniform(shared_keys[16], (HALF_DIM,), jnp.float32, 0.0, 3.5)),
        'expert_idx': expert_idx,
        'route_mask': route_mask,
    }


def layer_norm(x_in, gain_vec, bias_vec):
    x_f32 = x_in.astype(jnp.float32)
    mean_val = jnp.mean(x_f32, axis=-1, keepdims=True)
    centered = x_f32 - mean_val
    var_val = jnp.mean(centered * centered, axis=-1, keepdims=True)
    return (centered * lax.rsqrt(var_val + NORM_EPS) * gain_vec + bias_vec).astype(jnp.bfloat16)


def rotate_heads(x_in, angles):
    cos_half = jnp.cos(angles) * ROPE_MSCALE
    sin_half = jnp.sin(angles) * ROPE_MSCALE
    cos_full = jnp.concatenate([cos_half, cos_half], axis=-1)[:, None, :]
    sin_full = jnp.concatenate([sin_half, sin_half], axis=-1)[:, None, :]
    x_f32 = x_in.astype(jnp.float32)
    rotated = jnp.concatenate([-x_f32[..., HALF_DIM:], x_f32[..., :HALF_DIM]], axis=-1)
    return (x_f32 * cos_full + rotated * sin_full).astype(jnp.bfloat16)


def partial_stats(q_grp, keys, values, keep_mask):
    scores = jnp.einsum('bkgd,btkd->bkgt', q_grp.astype(jnp.float32), keys.astype(jnp.float32)) * (HEAD_DIM ** -0.5)
    keep_full = keep_mask[:, None, None, :]
    scores = jnp.where(keep_full, scores, NEG_FILL)
    run_max = jnp.max(scores, axis=-1)
    weights = jnp.where(keep_full, jnp.exp(scores - run_max[..., None]), 0.0)
    run_sum = jnp.sum(weights, axis=-1)
    out_part = jnp.einsum('bkgt,btkd->bkgd', weights.astype(jnp.bfloat16).astype(jnp.float32), values.astype(jnp.float32))
    return run_max, run_sum, out_part


def reference(x_first, next_emb, k_cache, v_cache, seq_len, ln1_gain, ln1_bias, w_q, b_q, w_k, b_k, w_v, b_v, w_o, b_o, ln2_gain, ln2_bias, w_router, w_gate, w_up, w_down, long_factor, expert_idx, route_mask):
    inv_freq = 1.0 / (long_factor * ROPE_BASE ** (jnp.arange(HALF_DIM, dtype=jnp.float32) * 2.0 / HEAD_DIM))
    step_inputs = jnp.concatenate([x_first[None], next_emb], axis=0)
    shard_ids = jnp.arange(KV_GROUP)
    tail_slots = jnp.arange(NUM_STEPS)

    def decode_step(step_carry, step_in):
        tail_k, tail_v = step_carry
        x_in, idx_step, mask_step, step_idx = step_in
        h_norm = layer_norm(x_in, ln1_gain, ln1_bias)
        q_new = (jnp.dot(h_norm, w_q, preferred_element_type=jnp.float32) + b_q).astype(jnp.bfloat16).reshape(BATCH_SIZE, Q_HEADS, HEAD_DIM)
        k_new = (jnp.dot(h_norm, w_k, preferred_element_type=jnp.float32) + b_k).astype(jnp.bfloat16).reshape(BATCH_SIZE, KV_HEADS, HEAD_DIM)
        v_new = (jnp.dot(h_norm, w_v, preferred_element_type=jnp.float32) + b_v).astype(jnp.bfloat16).reshape(BATCH_SIZE, KV_HEADS, HEAD_DIM)
        angles = (seq_len + step_idx).astype(jnp.float32)[:, None] * inv_freq[None, :]
        q_grp = rotate_heads(q_new, angles).reshape(BATCH_SIZE, KV_HEADS, Q_GROUP, HEAD_DIM)
        k_rot = rotate_heads(k_new, angles)
        tail_k = lax.dynamic_update_slice_in_dim(tail_k, k_rot[:, None], step_idx, axis=1)
        tail_v = lax.dynamic_update_slice_in_dim(tail_v, v_new[:, None], step_idx, axis=1)

        def one_shard(shard_id):
            k_blk = lax.dynamic_slice_in_dim(k_cache, shard_id * SHARD_LEN, SHARD_LEN, axis=1)
            v_blk = lax.dynamic_slice_in_dim(v_cache, shard_id * SHARD_LEN, SHARD_LEN, axis=1)
            positions = shard_id * SHARD_LEN + jnp.arange(SHARD_LEN)
            keep_mask = positions[None, :] < seq_len[:, None]
            return partial_stats(q_grp, k_blk, v_blk, keep_mask)

        cache_max, cache_sum, cache_out = lax.map(one_shard, shard_ids)
        tail_keep = jnp.broadcast_to(tail_slots[None, :] <= step_idx, (BATCH_SIZE, NUM_STEPS))
        tail_max, tail_sum, tail_out = partial_stats(q_grp, tail_k, tail_v, tail_keep)
        max_all = jnp.concatenate([cache_max, tail_max[None]], axis=0)
        sum_all = jnp.concatenate([cache_sum, tail_sum[None]], axis=0)
        out_all = jnp.concatenate([cache_out, tail_out[None]], axis=0)
        top_max = jnp.max(max_all, axis=0, keepdims=True)
        factor = jnp.exp(max_all - top_max)
        total_sum = jnp.sum(sum_all * factor, axis=0)
        merged = jnp.sum(out_all * factor[..., None], axis=0) / total_sum[..., None]
        attn_out = merged.reshape(BATCH_SIZE, Q_HEADS * HEAD_DIM).astype(jnp.bfloat16)
        x_mid = (x_in.astype(jnp.float32) + jnp.dot(attn_out, w_o, preferred_element_type=jnp.float32) + b_o).astype(jnp.bfloat16)
        h_moe = layer_norm(x_mid, ln2_gain, ln2_bias)
        logits = jnp.dot(h_moe, w_router, preferred_element_type=jnp.float32)
        masked = jnp.where(mask_step == 1, logits[:, None, :], NEG_FILL)
        gate_probs = jax.nn.softmax(masked, axis=-1)
        chosen = idx_step[..., None] == jnp.arange(NUM_EXPERTS)[None, None, :]
        gate_mat = jnp.sum(jnp.where(chosen, gate_probs, 0.0), axis=1)

        def expert_body(part_acc, expert_in):
            gate_w, up_w, down_w, gate_col = expert_in
            act_gate = jnp.dot(h_moe, gate_w, preferred_element_type=jnp.float32)
            act_up = jnp.dot(h_moe, up_w, preferred_element_type=jnp.float32)
            mixed_act = (gate_col[:, None] * jax.nn.silu(act_gate) * act_up).astype(jnp.bfloat16)
            blocks = mixed_act.reshape(BATCH_SIZE, KV_GROUP, FF_SHARD).astype(jnp.float32)
            down_blocks = down_w.reshape(KV_GROUP, FF_SHARD, D_MODEL).astype(jnp.float32)
            return part_acc + jnp.einsum('bjf,jfd->bjd', blocks, down_blocks), None

        part_init = jnp.zeros((BATCH_SIZE, KV_GROUP, D_MODEL), jnp.float32)
        part_acc = lax.scan(expert_body, part_init, (w_gate, w_up, w_down, gate_mat.T))[0]
        moe_out = jnp.sum(part_acc.astype(jnp.bfloat16).astype(jnp.float32), axis=1)
        x_out = (x_mid.astype(jnp.float32) + moe_out).astype(jnp.bfloat16)
        return (tail_k, tail_v), x_out

    tail_init = jnp.zeros((BATCH_SIZE, NUM_STEPS, KV_HEADS, HEAD_DIM), jnp.bfloat16)
    final_carry, hidden = lax.scan(decode_step, (tail_init, tail_init), (step_inputs, expert_idx, route_mask, jnp.arange(NUM_STEPS)))
    return hidden, final_carry[0], final_carry[1]
```

```python
import math
import jax
import jax.numpy as jnp
from jax import lax
from jax.sharding import PartitionSpec as P

ROPE_BASE = 10000.0
ROPE_MSCALE = math.sqrt(1.0 + math.log(32.0) / math.log(4096.0))
NORM_EPS = 1e-5
NEG_FILL = -1e30


def layer_norm(x_in, gain_vec, bias_vec):
    x_f32 = x_in.astype(jnp.float32)
    mean_val = jnp.mean(x_f32, axis=-1, keepdims=True)
    centered = x_f32 - mean_val
    var_val = jnp.mean(centered * centered, axis=-1, keepdims=True)
    return (centered * lax.rsqrt(var_val + NORM_EPS) * gain_vec + bias_vec).astype(jnp.bfloat16)


def rotate_heads(x_in, angles):
    half_dim = x_in.shape[-1] // 2
    cos_half = jnp.cos(angles) * ROPE_MSCALE
    sin_half = jnp.sin(angles) * ROPE_MSCALE
    cos_full = jnp.concatenate([cos_half, cos_half], axis=-1)[:, None, :]
    sin_full = jnp.concatenate([sin_half, sin_half], axis=-1)[:, None, :]
    x_f32 = x_in.astype(jnp.float32)
    rotated = jnp.concatenate([-x_f32[..., half_dim:], x_f32[..., :half_dim]], axis=-1)
    return (x_f32 * cos_full + rotated * sin_full).astype(jnp.bfloat16)


def inverse_freq(long_factor, head_dim):
    half_dim = head_dim // 2
    return 1.0 / (long_factor * ROPE_BASE ** (jnp.arange(half_dim, dtype=jnp.float32) * 2.0 / head_dim))


def partial_stats(q_grp, keys, values, keep_mask):
    scores = jnp.einsum('bkgd,btkd->bkgt', q_grp, keys, preferred_element_type=jnp.float32) * (q_grp.shape[-1] ** -0.5)
    keep_full = keep_mask
    scores = jnp.where(keep_full, scores, NEG_FILL)
    run_max = jnp.max(scores, axis=-1)
    weights = jnp.where(keep_full, jnp.exp(scores - run_max[..., None]), 0.0)
    run_sum = jnp.sum(weights, axis=-1)
    out_part = jnp.einsum('bkgt,btkd->bkgd', weights.astype(jnp.bfloat16), values, preferred_element_type=jnp.float32)
    return run_max, run_sum, out_part


def combine_stats(max_all, sum_all, out_all):
    top_max = jnp.max(max_all, axis=0, keepdims=True)
    factor = jnp.exp(max_all - top_max)
    total_sum = jnp.sum(sum_all * factor, axis=0)
    merged = jnp.sum(out_all * factor[..., None], axis=0)
    return jnp.concatenate([total_sum[..., None], merged], axis=-1)


def gate_matrix(h_moe, w_router, idx_step, mask_step):
    logits = jnp.dot(h_moe, w_router, preferred_element_type=jnp.float32)
    masked = jnp.where(mask_step == 1, logits[:, None, :], NEG_FILL)
    gate_probs = jax.nn.softmax(masked, axis=-1)
    chosen = idx_step[..., None] == jnp.arange(logits.shape[-1])[None, None, :]
    return jnp.sum(jnp.where(chosen, gate_probs, 0.0), axis=1)


def expert_part(h_moe, gate_mat, w_gate, w_up, w_down):
    act_gate = jnp.einsum('bd,edf->bef', h_moe, w_gate, preferred_element_type=jnp.float32)
    act_up = jnp.einsum('bd,edf->bef', h_moe, w_up, preferred_element_type=jnp.float32)
    mixed_act = (gate_mat[:, :, None] * jax.nn.silu(act_gate) * act_up).astype(jnp.bfloat16)
    return jnp.einsum('bef,efd->bd', mixed_act, w_down, preferred_element_type=jnp.float32).astype(jnp.bfloat16)


def solution(mesh):
    def layer_steps(x_first, next_emb, k_cache, v_cache, seq_len, ln1_gain, ln1_bias, w_q, b_q, w_k, b_k, w_v, b_v, w_o, b_o, ln2_gain, ln2_bias, w_router, w_gate, w_up, w_down, long_factor, expert_idx, route_mask):
        batch_rows, shard_len, kv_heads, head_dim = k_cache.shape
        q_heads = w_q.shape[1] // head_dim
        q_group = q_heads // kv_heads
        shard_id = lax.axis_index('kv')
        positions = shard_id * shard_len + jnp.arange(shard_len)
        cache_keep = positions[None, :] < seq_len[:, None]
        inv_freq = inverse_freq(long_factor, head_dim)
        num_steps = next_emb.shape[0] + 1
        width = x_first.shape[1]
        x_in = jnp.concatenate([x_first[None], next_emb], axis=0).reshape(num_steps * batch_rows, width)
        h_norm = layer_norm(x_in, ln1_gain, ln1_bias)
        q_new = (jnp.dot(h_norm, w_q, preferred_element_type=jnp.float32) + b_q).astype(jnp.bfloat16).reshape(-1, q_heads, head_dim)
        k_new = (jnp.dot(h_norm, w_k, preferred_element_type=jnp.float32) + b_k).astype(jnp.bfloat16).reshape(-1, kv_heads, head_dim)
        v_new = (jnp.dot(h_norm, w_v, preferred_element_type=jnp.float32) + b_v).astype(jnp.bfloat16).reshape(num_steps, batch_rows, kv_heads, head_dim)
        step_pos = seq_len[None, :] + jnp.arange(num_steps, dtype=seq_len.dtype)[:, None]
        angles = step_pos.reshape(-1).astype(jnp.float32)[:, None] * inv_freq[None, :]
        q_rot = rotate_heads(q_new, angles).reshape(num_steps, batch_rows, kv_heads, q_group, head_dim)
        q_grp = q_rot.transpose(1, 2, 0, 3, 4).reshape(batch_rows, kv_heads, num_steps * q_group, head_dim)
        tail_k = rotate_heads(k_new, angles).reshape(num_steps, batch_rows, kv_heads, head_dim).transpose(1, 0, 2, 3)
        tail_v = v_new.transpose(1, 0, 2, 3)
        run_max, run_sum, out_part = partial_stats(q_grp, k_cache, v_cache, cache_keep[:, None, None, :])
        row_step = jnp.arange(num_steps * q_group) // q_group
        tail_keep = jnp.arange(num_steps)[None, :] <= row_step[:, None]
        tail_max, tail_sum, tail_out = partial_stats(q_grp, tail_k, tail_v, tail_keep[None, None])
        packed = jnp.concatenate([run_max[..., None], run_sum[..., None], out_part], axis=-1)
        gathered = lax.all_to_all(packed.reshape((batch_rows,) + packed.shape[1:]), 'kv', 0, 0, tiled=True)
        group = lax.axis_size('kv')
        own = batch_rows // group
        gathered = gathered.reshape((group, own) + packed.shape[1:])
        own_tail = lambda arr: lax.dynamic_slice_in_dim(arr, shard_id * own, own, axis=0)[None]
        max_all = jnp.concatenate([gathered[..., 0], own_tail(tail_max)], axis=0)
        sum_all = jnp.concatenate([gathered[..., 1], own_tail(tail_sum)], axis=0)
        out_all = jnp.concatenate([gathered[..., 2:], own_tail(tail_out)], axis=0)
        merged = combine_stats(max_all, sum_all, out_all)
        merged = lax.all_gather(merged, 'kv', tiled=True)
        merged = merged[..., 1:] / merged[..., :1]
        merged = merged.reshape(batch_rows, kv_heads, num_steps, q_group, head_dim).transpose(2, 0, 1, 3, 4)
        attn_out = merged.reshape(num_steps * batch_rows, q_heads * head_dim).astype(jnp.bfloat16)
        x_mid = (x_in.astype(jnp.float32) + jnp.dot(attn_out, w_o, preferred_element_type=jnp.float32) + b_o).astype(jnp.bfloat16)
        h_moe = layer_norm(x_mid, ln2_gain, ln2_bias)
        top_k = expert_idx.shape[2]
        gate_mat = gate_matrix(h_moe, w_router, expert_idx.reshape(-1, top_k), route_mask.reshape(-1, top_k, route_mask.shape[3]))
        moe_part = expert_part(h_moe, gate_mat, w_gate, w_up, w_down)
        moe_sum = lax.psum(moe_part.astype(jnp.float32), 'kv')
        hidden = (x_mid.astype(jnp.float32) + moe_sum).astype(jnp.bfloat16)
        return hidden.reshape(num_steps, batch_rows, width), tail_k, tail_v

    replicated = P()
    in_specs = (P('dp'), P(None, 'dp'), P('dp', 'kv'), P('dp', 'kv'), P('dp')) + (replicated,) * 13 + (P(None, None, 'kv'), P(None, None, 'kv'), P(None, 'kv'), replicated, P(None, 'dp'), P(None, 'dp'))
    out_specs = (P(None, 'dp'), P('dp'), P('dp'))
    return jax.shard_map(layer_steps, mesh=mesh, in_specs=in_specs, out_specs=out_specs, check_vma=False)
```

```python
import functools
import math

import jax
import jax.numpy as jnp
import numpy as np
from jax import lax
from jax.experimental import pallas as pl
from jax.experimental.pallas import tpu as pltpu
from jax.sharding import PartitionSpec as P

ROPE_BASE = 10000.0
ROPE_MSCALE = math.sqrt(1.0 + math.log(32.0) / math.log(4096.0))
NORM_EPS = 1e-5
NEG_FILL = -1e30
MESH = pl.DeviceIdType.MESH
F32 = jnp.float32
BF16 = jnp.bfloat16
GROUPS = 2
K_CHUNKS = 8
TILE = 128


def iota(shape, dim):
    return lax.broadcasted_iota(jnp.int32, shape, dim)


def layer_norm_rows(x_f32, gain, bias):
    inv = 1.0 / x_f32.shape[-1]
    mean = jnp.sum(x_f32, axis=-1, keepdims=True) * inv
    centered = x_f32 - mean
    var = jnp.sum(centered * centered, axis=-1, keepdims=True) * inv
    return (centered * lax.rsqrt(var + NORM_EPS) * gain + bias).astype(BF16)


def dot_nt(a, b):
    return lax.dot_general(a, b, (((1,), (1,)), ((), ())), preferred_element_type=F32)


def dot_nn(a, b):
    return jnp.dot(a, b, preferred_element_type=F32)


def kernel(
    group,
    x_first, next_emb, kc, vc, seq_len, ln1_g, ln1_b, wq, bq, wk, bk, wv, bv, wo, bo, ln2_g, ln2_b, wr,
    wg, wu, wd, long_factor, powers, idx, mask,
    hidden, tail_k, tail_v,
    xbuf, hbuf, ln1g_v, ln1b_v, ln2g_v, ln2b_v, bo_v, bq_v, bk_v, bv_v, lf_v, pw_v, wr_v, idx_v, mask_v,
    wq_v, wk_v, wv_v, kc_v, vc_v, wo_v, acc_q, acc_k, acc_v, q2, k2, v2, tcol,
    stat, d2d1, rs1_send, rs1, obuf, osum, xmid, h2, act_g, act_u, pbuf, d2d2, sbuf, rs2, ybuf,
    small_sem, qkv_sem, kv_sem, wo_sem, moe_sem,
    d2d1_sem, rs1_sem, ag1_sem, fw1_sem, d2d2_sem, rs2_sem, ag2_sem, fw2_sem,
):
    batch, width = x_first.shape
    steps = next_emb.shape[0] + 1
    rows = steps * batch
    chips = group // 2
    q_heads = wq.shape[1] // TILE
    kv_heads = wk.shape[1] // TILE
    nb = batch // GROUPS
    spc = nb // chips
    rg = steps * nb
    half = q_heads * steps // 2
    qrows = 2 * half
    keys = kc.shape[1]
    shard_len = keys // kv_heads
    kstep = width // K_CHUNKS
    ff = wg.shape[0]
    experts = wr.shape[0]
    block = width // group
    scale = TILE ** -0.5

    me = lax.axis_index("kv")
    chip = lax.div(me, 2)
    core = lax.rem(me, 2)
    partner = me + 1 - 2 * core
    other = 1 - core

    def peer_chip(d):
        return lax.rem(chip + d, chips)

    def peer(d):
        return peer_chip(d) * 2 + core

    order = sorted(range(1, chips), key=lambda d: -min(d, chips - d))
    arrive = sorted(range(1, chips), key=lambda d: min(d, chips - d))

    barrier = pltpu.get_barrier_semaphore()
    pl.semaphore_signal(barrier, inc=1, device_id={"kv": partner}, device_id_type=MESH)
    for d in order:
        pl.semaphore_signal(barrier, inc=1, device_id={"kv": peer(d)}, device_id_type=MESH)

    smalls = [
        (x_first, xbuf.at[0]), (next_emb, xbuf.at[pl.ds(1, steps - 1)]), (ln1_g, ln1g_v), (ln1_b, ln1b_v),
        (long_factor, lf_v), (powers, pw_v), (bq, bq_v), (bk, bk_v), (bv, bv_v), (bo, bo_v),
        (ln2_g, ln2g_v), (ln2_b, ln2b_v), (wr, wr_v), (idx, idx_v), (mask, mask_v),
    ]
    small_copies = [pltpu.make_async_copy(src, dst, small_sem.at[i]) for i, (src, dst) in enumerate(smalls)]
    for copy in small_copies[:6]:
        copy.start()

    def qkv_copies(k):
        span = pl.ds(k * kstep, kstep)
        return [
            pltpu.make_async_copy(wq.at[span], wq_v.at[k], qkv_sem.at[0, k]),
            pltpu.make_async_copy(wk.at[span], wk_v.at[k], qkv_sem.at[1, k]),
            pltpu.make_async_copy(wv.at[span], wv_v.at[k], qkv_sem.at[2, k]),
        ]

    for k in range(K_CHUNKS):
        for copy in qkv_copies(k):
            copy.start()
    for copy in small_copies[6:]:
        copy.start()
    kv_copies = []
    for g in range(GROUPS):
        span = pl.ds(g * nb, nb)
        kv_copies.append([
            pltpu.make_async_copy(kc.at[span], kc_v.at[span], kv_sem.at[0, g]),
            pltpu.make_async_copy(vc.at[span], vc_v.at[span], kv_sem.at[1, g]),
        ])
        for copy in kv_copies[-1]:
            copy.start()
    wo_copy = pltpu.make_async_copy(wo, wo_v, wo_sem.at[0])
    wo_copy.start()

    row_k = iota((qrows, keys), 0)
    col_k = iota((qrows, keys), 1)
    head_of_row = (row_k * 43) >> 9
    pos = me * shard_len + (col_k >> 2)
    tcol[...] = jnp.where(head_of_row == (col_k & 3), pos, jnp.int32(1 << 30))

    for copy in small_copies[:6]:
        copy.wait()
    lane = iota((batch, TILE), 1)
    sub = iota((batch, TILE), 0)
    lens = jnp.zeros((batch, TILE), jnp.int32)
    for b in range(batch):
        lens = jnp.where(sub == b, seq_len[b], lens)
    lf = jnp.concatenate([lf_v[...], lf_v[...]], axis=1)
    inv_freq = 1.0 / (lf * pw_v[...])
    sign = jnp.where(lane < TILE // 2, -1.0, 1.0)
    cos_parts, sin_parts = [], []
    for s in range(steps):
        angles = (lens + s).astype(F32) * inv_freq
        cos_parts.append(jnp.cos(angles) * ROPE_MSCALE)
        sin_parts.append(jnp.sin(angles) * ROPE_MSCALE * sign)
    cos_full = jnp.concatenate(cos_parts, axis=0)
    sin_full = jnp.concatenate(sin_parts, axis=0)

    for s in range(steps):
        hbuf[s] = layer_norm_rows(xbuf[s].astype(F32), ln1g_v[...], ln1b_v[...])

    acc_q[...] = jnp.zeros_like(acc_q)
    acc_k[...] = jnp.zeros_like(acc_k)
    acc_v[...] = jnp.zeros_like(acc_v)

    @pl.loop(0, K_CHUNKS)
    def _(k):
        for copy in qkv_copies(k):
            copy.wait()
        h = hbuf[:, :, pl.ds(pl.multiple_of(k * kstep, kstep), kstep)].reshape(rows, kstep)
        acc_q[...] += dot_nn(h, wq_v[k])
        acc_k[...] += dot_nn(h, wk_v[k])
        acc_v[...] += dot_nn(h, wv_v[k])

    moe_copies = []
    hw = width // 2
    for i, src in enumerate((wg, wu, wd)):
        for j in range(2):
            copy = pltpu.make_async_copy(src.at[:, pl.ds(j * hw, hw)], wq_v.at[2 * i + j, pl.ds(0, ff)], moe_sem.at[i, j])
            copy.start()
            moe_copies.append(copy)
    for copy in small_copies[6:]:
        copy.wait()

    def rotate(x):
        x = x.astype(BF16).astype(F32)
        return (x * cos_full + pltpu.roll(x, TILE // 2, 1) * sin_full).astype(BF16).astype(F32)

    for i in range(q_heads):
        cols = pl.ds(i * TILE, TILE)
        q2[pl.ds(i * rows, rows)] = rotate(acc_q[:, cols] + bq_v[:, cols])
    for i in range(kv_heads):
        cols = pl.ds(i * TILE, TILE)
        k_rot = rotate(acc_k[:, cols] + bk_v[:, cols])
        v_new = (acc_v[:, cols] + bv_v[:, cols]).astype(BF16)
        k2[pl.ds(i * rows, rows)] = k_rot
        v2[pl.ds(i * rows, rows)] = v_new.astype(F32)
        for s in range(steps):
            tail_k[i, s] = k_rot[s * batch:(s + 1) * batch].astype(BF16)
            tail_v[i, s] = v_new[s * batch:(s + 1) * batch]
    k2[pl.ds(kv_heads * rows, k2.shape[0] - kv_heads * rows)] = jnp.zeros((k2.shape[0] - kv_heads * rows, TILE), F32)
    v2[pl.ds(kv_heads * rows, v2.shape[0] - kv_heads * rows)] = jnp.zeros((v2.shape[0] - kv_heads * rows, TILE), F32)

    eye = iota((half, TILE), 0) == iota((half, TILE), 1)
    sub8 = iota((8, TILE), 0)

    def to_row(col):
        return jnp.sum(jnp.where(eye, jnp.broadcast_to(col, (half, TILE)), 0.0), axis=0, keepdims=True)

    def to_col(row):
        return jnp.sum(jnp.where(eye, jnp.broadcast_to(row, (half, TILE)), 0.0), axis=1, keepdims=True)

    def pair_tile(m_row, l_row):
        return jnp.where(sub8 == 0, m_row, jnp.where(sub8 == 1, l_row, 0.0))

    def attend(b):
        q = q2[pl.ds(b, qrows, stride=batch)].astype(BF16)
        scores = dot_nt(q, kc_v[b]) * scale
        keep = tcol[...] < seq_len[b]
        scores = jnp.where(keep, scores, NEG_FILL)
        top = jnp.max(scores, axis=1, keepdims=True)
        w = jnp.where(keep, jnp.exp(scores - top), 0.0)
        total = jnp.sum(w, axis=1, keepdims=True)
        out = dot_nn(w.astype(BF16), vc_v[b])
        for hf in range(2):
            part = slice(hf * half, (hf + 1) * half)
            stat[hf, b, pl.ds(0, half)] = out[part]
            stat[hf, b, pl.ds(half, 8)] = pair_tile(to_row(top[part]), to_row(total[part]))

    sends = []

    def send(src, dst, sems, slot, device):
        copy = pltpu.make_async_remote_copy(
            src_ref=src, dst_ref=dst, send_sem=sems.at[(0,) + slot], recv_sem=sems.at[(1,) + slot],
            device_id={"kv": device}, device_id_type=MESH)
        copy.start()
        sends.append(copy)
        return copy

    d2d1_copies, rs1_copies, ag1_copies, fw1_copies = {}, {}, {}, {}
    d2d2_copies, rs2_copies, ag2_copies, fw2_copies = {}, {}, {}, {}

    def merge_pair(b):
        own, got = stat[core, b], d2d1[b]
        m1, l1 = own[half:half + 1], own[half + 1:half + 2]
        m2, l2 = got[half:half + 1], got[half + 1:half + 2]
        top = jnp.maximum(m1, m2)
        a1, a2 = jnp.exp(m1 - top), jnp.exp(m2 - top)
        rs1_send[b, pl.ds(0, half)] = own[:half] * to_col(a1) + got[:half] * to_col(a2)
        rs1_send[b, pl.ds(half, 8)] = pair_tile(top, l1 * a1 + l2 * a2)

    def start_d2d1(g):
        span = pl.ds(g * nb, nb)
        d2d1_copies[g] = send(stat.at[other, span], d2d1.at[span], d2d1_sem, (g,), partner)

    def start_rs1(g):
        d2d1_copies[g].wait_recv()
        for i in range(nb):
            merge_pair(g * nb + i)
        for d in order:
            span = pl.ds(g * nb + peer_chip(d) * spc, spc)
            rs1_copies[g, d] = send(rs1_send.at[span], rs1.at[g, d], rs1_sem, (g, d), peer(d))

    def tail_stats(b):
        q = q2[pl.ds(b + core * (half * batch), half, stride=batch)].astype(BF16)
        k = k2[pl.ds(b, 16, stride=batch)].astype(BF16)
        v = v2[pl.ds(b, 16, stride=batch)].astype(BF16)
        r, j = iota((half, 16), 0), iota((half, 16), 1)
        r3, j3 = (r * 43) >> 7, (j * 43) >> 7
        head = core * (kv_heads // 2) + (r3 >> 2)
        keep = (j3 == head) & ((j - j3 * steps) <= (r - r3 * steps))
        scores = jnp.where(keep, dot_nt(q, k) * scale, NEG_FILL)
        top = jnp.max(scores, axis=1, keepdims=True)
        w = jnp.where(keep, jnp.exp(scores - top), 0.0)
        total = jnp.sum(w, axis=1, keepdims=True)
        return dot_nn(w.astype(BF16), v), to_row(top), to_row(total)

    def start_ag1(g):
        tails = [tail_stats(g * nb + chip * spc + i) for i in range(spc)]
        for d in arrive:
            rs1_copies[g, d].wait_recv()
        for i in range(spc):
            b = g * nb + chip * spc + i
            own = rs1_send[b]
            units = [tails[i], (own[:half], own[half:half + 1], own[half + 1:half + 2])]
            for d in arrive:
                got = rs1[g, d, i]
                units.append((got[:half], got[half:half + 1], got[half + 1:half + 2]))
            top = functools.reduce(jnp.maximum, [u[1] for u in units])
            o_sum, l_sum = 0.0, 0.0
            for o, m, l in units:
                a = jnp.exp(m - top)
                l_sum = l_sum + l * a
                o_sum = o_sum + o * to_col(a)
            obuf[g, core, chip, i] = o_sum / to_col(l_sum)
        own_ref = obuf.at[g, core, chip]
        for d in order:
            ag1_copies[g, d] = send(own_ref, own_ref, ag1_sem, (g, d), peer(d))
        fw1_copies[g, 0] = send(own_ref, own_ref, fw1_sem, (g, 0), partner)

    def forward1(g):
        for d in arrive:
            ag1_copies[g, d].wait_recv()
            ref = obuf.at[g, core, peer_chip(chips - d)]
            fw1_copies[g, d] = send(ref, ref, fw1_sem, (g, d), partner)

    def finish1(g):
        for d in range(chips):
            fw1_copies[g, d].wait_recv()
        for hf in range(2):
            for i in range(q_heads // 2):
                parts = []
                for s in range(steps):
                    parts.append(osum_rows(g, hf, i * steps + s))
                col = hf * (q_heads // 2) + i
                osum[:, pl.ds(col * TILE, TILE)] = jnp.concatenate(parts, axis=0)

    def osum_rows(g, hf, r):
        return obuf_rows.at[g, hf][pl.ds(r, nb, stride=half)]

    obuf_rows = obuf.reshape(GROUPS, 2, nb * half, TILE)

    def project(g):
        o = osum[...].astype(BF16)
        x = xbuf[:, pl.ds(g * nb, nb)].astype(F32).reshape(rg, width)
        xmid[g] = x

        @pl.loop(0, K_CHUNKS)
        def _(n):
            cols = pl.ds(pl.multiple_of(n * kstep, kstep), kstep)
            val = xmid[g, :, cols] + dot_nn(o, wo_v[:, cols]) + bo_v[:, cols]
            xmid[g, :, cols] = val.astype(BF16).astype(F32)

        h2[...] = layer_norm_rows(xmid[g], ln2g_v[...], ln2b_v[...])

    def gates(g):
        logits = dot_nt(h2[...], wr_v[...])
        out = []
        e = iota((nb, experts), 1)
        pick = iota((nb, batch), 1) == iota((nb, batch), 0) + g * nb
        for s in range(steps):
            r = logits[s * nb:(s + 1) * nb]
            total = jnp.zeros((nb, experts), F32)
            for k in range(idx_v.shape[1]):
                allowed = mask_v[s, pl.ds(g * nb, nb), k, :] == 1
                masked = jnp.where(allowed, r, NEG_FILL)
                p = jnp.exp(masked - jnp.max(masked, axis=1, keepdims=True))
                p = p / jnp.sum(p, axis=1, keepdims=True)
                row = jnp.broadcast_to(idx_v[s, pl.ds(k, 1), :].astype(F32), (nb, batch))
                col = jnp.sum(jnp.where(pick, row, 0.0), axis=1, keepdims=True)
                total = total + jnp.where(col == e.astype(F32), p, 0.0)
            out.append(total)
        gate = jnp.concatenate(out, axis=0)
        gate = jnp.concatenate([gate, jnp.zeros((rg, TILE - experts), F32)], axis=1)
        shift = experts
        while shift < TILE:
            gate = gate + pltpu.roll(gate, shift, 1)
            shift *= 2
        reps = -(-ff // TILE)
        return jnp.concatenate([gate] * reps, axis=1)[:, :ff]

    def expert_parts(g):
        gate = gates(g)
        act_g[...] = jnp.zeros_like(act_g)
        act_u[...] = jnp.zeros_like(act_u)
        per = K_CHUNKS // 2

        @pl.loop(0, 2)
        def _(j):
            @pl.loop(0, per)
            def _(k):
                src = pl.ds(pl.multiple_of(j * hw + k * kstep, kstep), kstep)
                cols = pl.ds(pl.multiple_of(k * kstep, kstep), kstep)
                h = h2[:, src]
                act_g[...] += dot_nt(h, wq_v[j, pl.ds(0, ff), cols])
                act_u[...] += dot_nt(h, wq_v[2 + j, pl.ds(0, ff), cols])

        ag = act_g[...]
        u = (gate * (ag * (1.0 / (1.0 + jnp.exp(-ag)))) * act_u[...]).astype(BF16)

        @pl.loop(0, 2)
        def _(j):
            @pl.loop(0, per)
            def _(k):
                cols = pl.ds(pl.multiple_of(k * kstep, kstep), kstep)
                part = dot_nn(u, wq_v[4 + j, pl.ds(0, ff), cols]).astype(BF16).astype(F32)
                pair = j * per + k
                pbuf[g, 0, pair] = part[:, :block]
                pbuf[g, 1, pair] = part[:, block:]

        d2d2_copies[g] = send(pbuf.at[g, other], d2d2.at[g], d2d2_sem, (g,), partner)

    def start_rs2(g):
        d2d2_copies[g].wait_recv()
        for d in order:
            z = peer_chip(d)
            sbuf[g, z] = pbuf[g, core, z] + d2d2[g, z]
            rs2_copies[g, d] = send(sbuf.at[g, z], rs2.at[g, d], rs2_sem, (g, d), peer(d))

    def start_ag2(g):
        total = pbuf[g, core, chip] + d2d2[g, chip]
        for d in arrive:
            rs2_copies[g, d].wait_recv()
            total = total + rs2[g, d]
        x = xmid[g, :, pl.ds(pl.multiple_of(me * block, block), block)]
        ybuf[g, core, chip] = (x + total).astype(BF16).astype(F32)
        own_ref = ybuf.at[g, core, chip]
        for d in order:
            ag2_copies[g, d] = send(own_ref, own_ref, ag2_sem, (g, d), peer(d))
        fw2_copies[g, 0] = send(own_ref, own_ref, fw2_sem, (g, 0), partner)

    def forward2(g):
        for d in arrive:
            ag2_copies[g, d].wait_recv()
            ref = ybuf.at[g, core, peer_chip(chips - d)]
            fw2_copies[g, d] = send(ref, ref, fw2_sem, (g, d), partner)

    for g in range(GROUPS):
        for copy in kv_copies[g]:
            copy.wait()

        @pl.loop(0, nb // 4)
        def _(i):
            for j in range(4):
                attend(g * nb + i * 4 + j)

        if g == 0:
            pl.semaphore_wait(barrier, chips)
        start_d2d1(g)
        if g > 0:
            start_rs1(g - 1)
    start_rs1(GROUPS - 1)
    for g in range(GROUPS):
        start_ag1(g)
    wo_copy.wait()
    for copy in moe_copies:
        copy.wait()
    for g in range(GROUPS):
        forward1(g)
        finish1(g)
        project(g)
        expert_parts(g)
        start_rs2(g)
    for g in range(GROUPS):
        start_ag2(g)
    for g in range(GROUPS):
        forward2(g)
    for g in range(GROUPS):
        for d in range(chips):
            fw2_copies[g, d].wait_recv()
    for z in range(chips):
        for c in range(2):
            cols = pl.ds((z * 2 + c) * block, block)
            for s in range(steps):
                parts = [ybuf[g, c, z, pl.ds(s * nb, nb)] for g in range(GROUPS)]
                hidden[s, :, cols] = jnp.concatenate(parts, axis=0).astype(BF16)
    for copy in sends:
        copy.wait_send()


def solution(mesh):
    group = mesh.shape["kv"]
    chips = group // 2

    def layer_steps(x_first, next_emb, k_cache, v_cache, seq_len, ln1_gain, ln1_bias, w_q, b_q, w_k, b_k, w_v, b_v, w_o, b_o, ln2_gain, ln2_bias, w_router, w_gate, w_up, w_down, long_factor, expert_idx, route_mask):
        batch, shard_len, kv_heads, head_dim = k_cache.shape
        width = x_first.shape[1]
        steps = next_emb.shape[0] + 1
        q_heads = w_q.shape[1] // head_dim
        experts, _, ff_local = w_gate.shape
        ff = experts * ff_local
        rows = steps * batch
        half = q_heads * steps // 2
        keys = shard_len * kv_heads
        nb = batch // GROUPS
        spc = nb // chips
        rg = steps * nb
        block = width // group
        kstep = width // K_CHUNKS
        exponent = np.arange(head_dim // 2, dtype=np.float64) * 2.0 / head_dim
        powers = np.tile((ROPE_BASE ** exponent).astype(np.float32), 2)[None]

        row = lambda vec: vec.reshape(1, -1)
        flat = lambda arr: arr.reshape(batch, keys, head_dim)
        operands = (
            x_first, next_emb, flat(k_cache), flat(v_cache), seq_len, row(ln1_gain), row(ln1_bias),
            w_q, row(b_q), w_k, row(b_k), w_v, row(b_v), w_o, row(b_o), row(ln2_gain), row(ln2_bias), w_router.T,
            w_gate.transpose(2, 0, 1).reshape(ff, width), w_up.transpose(2, 0, 1).reshape(ff, width),
            w_down.transpose(1, 0, 2).reshape(ff, width), row(long_factor), jnp.asarray(powers),
            expert_idx.transpose(0, 2, 1), route_mask,
        )
        any_spec = pl.BlockSpec(memory_space=pl.ANY)
        in_specs = [any_spec] * len(operands)
        in_specs[4] = pl.BlockSpec(memory_space=pltpu.SMEM)
        vmem = pl.BlockSpec(memory_space=pltpu.VMEM)
        V = pltpu.VMEM
        dma = pltpu.SemaphoreType.DMA
        scratch = [
            V((steps, batch, width), BF16), V((steps, batch, width), BF16),
            V((1, width), F32), V((1, width), F32), V((1, width), F32), V((1, width), F32), V((1, width), F32),
            V((1, q_heads * head_dim), F32), V((1, kv_heads * head_dim), F32), V((1, kv_heads * head_dim), F32),
            V((1, head_dim // 2), F32), V((1, head_dim), F32), V((experts, width), BF16),
            V((steps, expert_idx.shape[2], batch), jnp.int32), V(route_mask.shape, jnp.int32),
            V((K_CHUNKS, kstep, q_heads * head_dim), BF16),
            V((K_CHUNKS, kstep, kv_heads * head_dim), BF16), V((K_CHUNKS, kstep, kv_heads * head_dim), BF16),
            V((batch, keys, head_dim), BF16), V((batch, keys, head_dim), BF16), V(w_o.shape, BF16),
            V((rows, q_heads * head_dim), F32), V((rows, kv_heads * head_dim), F32), V((rows, kv_heads * head_dim), F32),
            V((q_heads * rows, head_dim), F32), V((16 * batch, head_dim), F32), V((16 * batch, head_dim), F32),
            V((2 * half, keys), jnp.int32),
            V((2, batch, half + 8, head_dim), F32), V((batch, half + 8, head_dim), F32), V((batch, half + 8, head_dim), F32),
            V((GROUPS, chips, spc, half + 8, head_dim), F32), V((GROUPS, 2, chips, spc, half, head_dim), F32),
            V((rg, q_heads * head_dim), F32), V((GROUPS, rg, width), F32), V((rg, width), BF16),
            V((rg, ff), F32), V((rg, ff), F32),
            V((GROUPS, 2, chips, rg, block), F32), V((GROUPS, chips, rg, block), F32), V((GROUPS, chips, rg, block), F32),
            V((GROUPS, chips, rg, block), F32), V((GROUPS, 2, chips, rg, block), F32),
            dma((15,)), dma((3, K_CHUNKS)), dma((2, GROUPS)), dma((1,)), dma((3, 2)),
            dma((2, GROUPS)), dma((2, GROUPS, chips)), dma((2, GROUPS, chips)), dma((2, GROUPS, chips)),
            dma((2, GROUPS)), dma((2, GROUPS, chips)), dma((2, GROUPS, chips)), dma((2, GROUPS, chips)),
        ]
        tail_shape = jax.ShapeDtypeStruct((kv_heads, steps, batch, head_dim), BF16)
        hidden, tail_k, tail_v = pl.pallas_call(
            functools.partial(kernel, group),
            out_shape=(jax.ShapeDtypeStruct((steps, batch, width), BF16), tail_shape, tail_shape),
            in_specs=in_specs,
            out_specs=(vmem, vmem, vmem),
            scratch_shapes=scratch,
            name="decode_layer",
            compiler_params=pltpu.CompilerParams(
                collective_id=0, has_side_effects=True, vmem_limit_bytes=66_000_000),
        )(*operands)
        order = (2, 1, 0, 3)
        return hidden, tail_k.transpose(order), tail_v.transpose(order)

    replicated = P()
    in_specs = (P('dp'), P(None, 'dp'), P('dp', 'kv'), P('dp', 'kv'), P('dp')) + (replicated,) * 13 + (P(None, None, 'kv'), P(None, None, 'kv'), P(None, 'kv'), replicated, P(None, 'dp'), P(None, 'dp'))
    out_specs = (P(None, 'dp'), P('dp'), P('dp'))
    return jax.shard_map(layer_steps, mesh=mesh, in_specs=in_specs, out_specs=out_specs, check_vma=False)
```

```python
import contextlib
import functools
import math

import jax
import jax.numpy as jnp
import numpy as np
from jax import lax
from jax.experimental import pallas as pl
from jax.experimental.pallas import tpu as pltpu
from jax.sharding import PartitionSpec as P

ROPE_BASE = 10000.0
ROPE_MSCALE = math.sqrt(1.0 + math.log(32.0) / math.log(4096.0))
NORM_EPS = 1e-5
NEG_FILL = -1e30
MESH = pl.DeviceIdType.MESH
F32 = jnp.float32
BF16 = jnp.bfloat16
GROUPS = 2
CHUNKS = 4
scope = contextlib.nullcontext
K_CHUNKS = 8
TILE = 128


def iota(shape, dim):
    return lax.broadcasted_iota(jnp.int32, shape, dim)


def layer_norm_rows(x_f32, gain, bias):
    inv = 1.0 / x_f32.shape[-1]
    mean = jnp.sum(x_f32, axis=-1, keepdims=True) * inv
    centered = x_f32 - mean
    var = jnp.sum(centered * centered, axis=-1, keepdims=True) * inv
    return (centered * lax.rsqrt(var + NORM_EPS) * gain + bias).astype(BF16)


def dot_nt(a, b):
    return lax.dot_general(a, b, (((1,), (1,)), ((), ())), preferred_element_type=F32)


def dot_nn(a, b):
    return jnp.dot(a, b, preferred_element_type=F32)


def kernel(
    group,
    x_first, next_emb, kc, vc, seq_len, ln1_g, ln1_b, wq, bq, wk, bk, wv, bv, wo, bo, ln2_g, ln2_b, wr,
    wg, wu, wd, long_factor, powers, idx, mask,
    hidden, tail_k, tail_v,
    xbuf, hbuf, ln1g_v, ln1b_v, ln2g_v, ln2b_v, bo_v, bq_v, bk_v, bv_v, lf_v, pw_v, wr_v, idx_v, mask_v,
    wq_v, wk_v, wv_v, kc_v, vc_v, wo_v, acc_q, acc_k, acc_v, q2, k2, v2, tcol,
    stat, d2d1, rs1_send, rs1, obuf, osum, xmid, h2, pbuf, d2d2, sbuf, rs2, ybuf,
    small_sem, qkv_sem, kv_sem, wo_sem, moe_sem,
    d2d1_sem, rs1_sem, ag1_sem, fw1_sem, d2d2_sem, rs2_sem, ag2_sem, fw2_sem,
):
    batch, width = x_first.shape
    steps = next_emb.shape[0] + 1
    rows = steps * batch
    chips = group // 2
    q_heads = wq.shape[1] // TILE
    kv_heads = wk.shape[1] // TILE
    nb = batch // GROUPS
    spc = nb // chips
    half = q_heads * steps // 2
    qrows = 2 * half
    keys = kc.shape[1]
    shard_len = keys // kv_heads
    kstep = width // K_CHUNKS
    ff = wg.shape[0]
    experts = wr.shape[0]
    block = width // group // 2
    scale = TILE ** -0.5

    me = lax.axis_index("kv")
    chip = lax.div(me, 2)
    core = lax.rem(me, 2)
    partner = me + 1 - 2 * core
    other = 1 - core

    def peer_chip(d):
        return lax.rem(chip + d, chips)

    def peer(d):
        return peer_chip(d) * 2 + core

    order = sorted(range(1, chips), key=lambda d: -min(d, chips - d))
    arrive = sorted(range(1, chips), key=lambda d: min(d, chips - d))

    barrier = pltpu.get_barrier_semaphore()
    pl.semaphore_signal(barrier, inc=1, device_id={"kv": partner}, device_id_type=MESH)
    for d in order:
        pl.semaphore_signal(barrier, inc=1, device_id={"kv": peer(d)}, device_id_type=MESH)

    smalls = [
        (x_first, xbuf.at[0]), (next_emb, xbuf.at[pl.ds(1, steps - 1)]), (ln1_g, ln1g_v), (ln1_b, ln1b_v),
        (long_factor, lf_v), (powers, pw_v), (bq, bq_v), (bk, bk_v), (bv, bv_v), (bo, bo_v),
        (ln2_g, ln2g_v), (ln2_b, ln2b_v), (wr, wr_v), (idx, idx_v), (mask, mask_v),
    ]
    small_copies = [pltpu.make_async_copy(src, dst, small_sem.at[i]) for i, (src, dst) in enumerate(smalls)]
    for copy in small_copies[:6]:
        copy.start()

    def qkv_copies(k):
        span = pl.ds(k * kstep, kstep)
        return [
            pltpu.make_async_copy(wq.at[span], wq_v.at[k], qkv_sem.at[0, k]),
            pltpu.make_async_copy(wk.at[span], wk_v.at[k], qkv_sem.at[1, k]),
            pltpu.make_async_copy(wv.at[span], wv_v.at[k], qkv_sem.at[2, k]),
        ]

    for copy in small_copies[6:]:
        copy.start()
    for k in range(K_CHUNKS):
        for copy in qkv_copies(k):
            copy.start(priority=1)
    kv_copies = []
    for g in range(GROUPS):
        span = pl.ds(g * nb, nb)
        kv_copies.append([
            pltpu.make_async_copy(kc.at[span], kc_v.at[span], kv_sem.at[0, g]),
            pltpu.make_async_copy(vc.at[span], vc_v.at[span], kv_sem.at[1, g]),
        ])
        for copy in kv_copies[-1]:
            copy.start(priority=1)
    wo_copy = pltpu.make_async_copy(wo, wo_v, wo_sem.at[0])
    wo_copy.start(priority=1)

    row_k = iota((qrows, keys), 0)
    col_k = iota((qrows, keys), 1)
    head_of_row = (row_k * 43) >> 9
    pos = me * shard_len + (col_k >> 2)
    tcol[...] = jnp.where(head_of_row == (col_k & 3), pos, jnp.int32(1 << 30))

    for copy in small_copies[:6]:
        copy.wait()
    lane = iota((batch, TILE), 1)
    sub = iota((batch, TILE), 0)
    lens = jnp.zeros((batch, TILE), jnp.int32)
    for b in range(batch):
        lens = jnp.where(sub == b, seq_len[b], lens)
    lf = jnp.concatenate([lf_v[...], lf_v[...]], axis=1)
    inv_freq = 1.0 / (lf * pw_v[...])
    sign = jnp.where(lane < TILE // 2, -1.0, 1.0)
    cos_parts, sin_parts = [], []
    for s in range(steps):
        angles = (lens + s).astype(F32) * inv_freq
        cos_parts.append(jnp.cos(angles) * ROPE_MSCALE)
        sin_parts.append(jnp.sin(angles) * ROPE_MSCALE * sign)
    cos_full = jnp.concatenate(cos_parts, axis=0)
    sin_full = jnp.concatenate(sin_parts, axis=0)

    for s in range(steps):
        hbuf[s] = layer_norm_rows(xbuf[s].astype(F32), ln1g_v[...], ln1b_v[...])

    acc_q[...] = jnp.zeros_like(acc_q)
    acc_k[...] = jnp.zeros_like(acc_k)
    acc_v[...] = jnp.zeros_like(acc_v)

    @pl.loop(0, K_CHUNKS)
    def _(k):
        for copy in qkv_copies(k):
            copy.wait()
        h = hbuf[:, :, pl.ds(pl.multiple_of(k * kstep, kstep), kstep)].reshape(rows, kstep)
        acc_q[...] += dot_nn(h, wq_v[k])
        acc_k[...] += dot_nn(h, wk_v[k])
        acc_v[...] += dot_nn(h, wv_v[k])

    moe_copies = []
    hw = width // 2
    for i, src in enumerate((wg, wu, wd)):
        for j in range(2):
            copy = pltpu.make_async_copy(src.at[:, pl.ds(j * hw, hw)], wq_v.at[2 * i + j, pl.ds(0, ff)], moe_sem.at[i, j])
            copy.start(priority=1)
            moe_copies.append(copy)
    for copy in small_copies[6:]:
        copy.wait()

    def rotate(x):
        x = x.astype(BF16).astype(F32)
        return (x * cos_full + pltpu.roll(x, TILE // 2, 1) * sin_full).astype(BF16).astype(F32)

    for i in range(q_heads):
        cols = pl.ds(i * TILE, TILE)
        q2[pl.ds(i * rows, rows)] = rotate(acc_q[:, cols] + bq_v[:, cols])
    for i in range(kv_heads):
        cols = pl.ds(i * TILE, TILE)
        k_rot = rotate(acc_k[:, cols] + bk_v[:, cols])
        v_new = (acc_v[:, cols] + bv_v[:, cols]).astype(BF16)
        k2[pl.ds(i * rows, rows)] = k_rot
        v2[pl.ds(i * rows, rows)] = v_new.astype(F32)
        tail_k[i] = k_rot
        tail_v[i] = v_new.astype(F32)
    k2[pl.ds(kv_heads * rows, k2.shape[0] - kv_heads * rows)] = jnp.zeros((k2.shape[0] - kv_heads * rows, TILE), F32)
    v2[pl.ds(kv_heads * rows, v2.shape[0] - kv_heads * rows)] = jnp.zeros((v2.shape[0] - kv_heads * rows, TILE), F32)

    eye = iota((half, TILE), 0) == iota((half, TILE), 1)
    sub8 = iota((8, TILE), 0)

    def to_row(col):
        return jnp.sum(jnp.where(eye, jnp.broadcast_to(col, (half, TILE)), 0.0), axis=0, keepdims=True)

    def to_col(row):
        return jnp.sum(jnp.where(eye, jnp.broadcast_to(row, (half, TILE)), 0.0), axis=1, keepdims=True)

    def pair_tile(m_row, l_row):
        return jnp.where(sub8 == 0, m_row, jnp.where(sub8 == 1, l_row, 0.0))

    def attend(b):
        q = q2[pl.ds(b, qrows, stride=batch)].astype(BF16)
        scores = dot_nt(q, kc_v[b]) * scale
        keep = tcol[...] < seq_len[b]
        scores = jnp.where(keep, scores, NEG_FILL)
        top = jnp.max(scores, axis=1, keepdims=True)
        w = jnp.where(keep, jnp.exp(scores - top), 0.0)
        total = jnp.sum(w, axis=1, keepdims=True)
        out = dot_nn(w.astype(BF16), vc_v[b])
        for hf in range(2):
            part = slice(hf * half, (hf + 1) * half)
            stat[hf, b, pl.ds(0, half)] = out[part]
            stat[hf, b, pl.ds(half, 8)] = pair_tile(to_row(top[part]), to_row(total[part]))

    sends = []

    def send(src, dst, sems, slot, device):
        copy = pltpu.make_async_remote_copy(
            src_ref=src, dst_ref=dst, send_sem=sems.at[(0,) + slot], recv_sem=sems.at[(1,) + slot],
            device_id={"kv": device}, device_id_type=MESH)
        copy.start()
        sends.append(copy)
        return copy

    d2d1_copies, rs1_copies, ag1_copies, fw1_copies = {}, {}, {}, {}
    d2d2_copies = {}

    def merge_pair(b):
        own, got = stat[core, b], d2d1[b]
        m1, l1 = own[half:half + 1], own[half + 1:half + 2]
        m2, l2 = got[half:half + 1], got[half + 1:half + 2]
        top = jnp.maximum(m1, m2)
        a1, a2 = jnp.exp(m1 - top), jnp.exp(m2 - top)
        rs1_send[b, pl.ds(0, half)] = own[:half] * to_col(a1) + got[:half] * to_col(a2)
        rs1_send[b, pl.ds(half, 8)] = pair_tile(top, l1 * a1 + l2 * a2)

    def start_d2d1(g):
        span = pl.ds(g * nb, nb)
        d2d1_copies[g] = send(stat.at[other, span], d2d1.at[span], d2d1_sem, (g,), partner)

    def start_rs1(g):
        d2d1_copies[g].wait_recv()
        for i in range(nb):
            merge_pair(g * nb + i)
        for d in order:
            span = pl.ds(g * nb + peer_chip(d) * spc, spc)
            rs1_copies[g, d] = send(rs1_send.at[span], rs1.at[g, d], rs1_sem, (g, d), peer(d))

    def tail_stats(b):
        q = q2[pl.ds(b + core * (half * batch), half, stride=batch)].astype(BF16)
        k = k2[pl.ds(b, 16, stride=batch)].astype(BF16)
        v = v2[pl.ds(b, 16, stride=batch)].astype(BF16)
        r, j = iota((half, 16), 0), iota((half, 16), 1)
        r3, j3 = (r * 43) >> 7, (j * 43) >> 7
        head = core * (kv_heads // 2) + (r3 >> 2)
        keep = (j3 == head) & ((j - j3 * steps) <= (r - r3 * steps))
        scores = jnp.where(keep, dot_nt(q, k) * scale, NEG_FILL)
        top = jnp.max(scores, axis=1, keepdims=True)
        w = jnp.where(keep, jnp.exp(scores - top), 0.0)
        total = jnp.sum(w, axis=1, keepdims=True)
        return dot_nn(w.astype(BF16), v), to_row(top), to_row(total)

    def start_ag1(g):
        tails = [tail_stats(g * nb + chip * spc + i) for i in range(spc)]
        for d in arrive:
            rs1_copies[g, d].wait_recv()
        for i in range(spc):
            b = g * nb + chip * spc + i
            own = rs1_send[b]
            units = [tails[i], (own[:half], own[half:half + 1], own[half + 1:half + 2])]
            for d in arrive:
                got = rs1[g, d, i]
                units.append((got[:half], got[half:half + 1], got[half + 1:half + 2]))
            top = functools.reduce(jnp.maximum, [u[1] for u in units])
            o_sum, l_sum = 0.0, 0.0
            for o, m, l in units:
                a = jnp.exp(m - top)
                l_sum = l_sum + l * a
                o_sum = o_sum + o * to_col(a)
            obuf[g, core, chip, i] = o_sum / to_col(l_sum)
        own_ref = obuf.at[g, core, chip]
        for d in order:
            ag1_copies[g, d] = send(own_ref, own_ref, ag1_sem, (g, d), peer(d))
        fw1_copies[g, 0] = send(own_ref, own_ref, fw1_sem, (g, 0), partner)

    def forward1(g):
        for d in arrive:
            ag1_copies[g, d].wait_recv()
            ref = obuf.at[g, core, peer_chip(chips - d)]
            fw1_copies[g, d] = send(ref, ref, fw1_sem, (g, d), partner)

    obuf_rows = obuf.reshape(GROUPS, 2, nb * half, TILE)

    def project():
        for hf in range(2):
            for i in range(q_heads // 2):
                parts = [obuf_rows.at[g, hf][pl.ds(i * steps + s, nb, stride=half)]
                         for s in range(steps) for g in range(GROUPS)]
                col = hf * (q_heads // 2) + i
                osum[:, pl.ds(col * TILE, TILE)] = jnp.concatenate(parts, axis=0)
        o = osum[...].astype(BF16)
        for n in range(2):
            cols = pl.ds(n * hw, hw)
            x = xbuf[:, :, cols].astype(F32).reshape(rows, hw)
            val = x + dot_nn(o, wo_v[:, cols]) + bo_v[:, cols]
            xmid[:, cols] = val.astype(BF16).astype(F32)
        h2[...] = layer_norm_rows(xmid[...], ln2g_v[...], ln2b_v[...])

    def gates():
        logits = dot_nt(h2[...], wr_v[...])
        out = []
        e = iota((batch, experts), 1).astype(F32)
        pick = iota((batch, batch), 1) == iota((batch, batch), 0)
        for s in range(steps):
            r = logits[s * batch:(s + 1) * batch]
            total = jnp.zeros((batch, experts), F32)
            for k in range(idx_v.shape[1]):
                masked = jnp.where(mask_v[s, :, k, :] == 1, r, NEG_FILL)
                p = jnp.exp(masked - jnp.max(masked, axis=1, keepdims=True))
                p = p / jnp.sum(p, axis=1, keepdims=True)
                row = jnp.broadcast_to(idx_v[s, pl.ds(k, 1), :].astype(F32), (batch, batch))
                col = jnp.sum(jnp.where(pick, row, 0.0), axis=1, keepdims=True)
                total = total + jnp.where(col == e, p, 0.0)
            out.append(total)
        gate = jnp.concatenate(out, axis=0)
        gate = jnp.concatenate([gate, jnp.zeros((rows, TILE - experts), F32)], axis=1)
        shift = experts
        while shift < TILE:
            gate = gate + pltpu.roll(gate, shift, 1)
            shift *= 2
        reps = -(-ff // TILE)
        return jnp.concatenate([gate] * reps, axis=1)[:, :ff]

    rhalf = rows // 2

    def expert_parts():
        gate = gates()
        span = pl.ds(0, ff)
        ag = dot_nt(h2[:, :hw], wq_v[0, span]) + dot_nt(h2[:, hw:], wq_v[1, span])
        au = dot_nt(h2[:, :hw], wq_v[2, span]) + dot_nt(h2[:, hw:], wq_v[3, span])
        u = (gate * (ag * (1.0 / (1.0 + jnp.exp(-ag)))) * au).astype(BF16)
        for h in range(2):
            part = dot_nn(u, wq_v[4 + h, span]).astype(BF16).astype(F32)
            for j in range(group):
                for r in range(2):
                    pbuf[2 * h + r, j % 2, j // 2] = part[r * rhalf:(r + 1) * rhalf, j * block:(j + 1) * block]
            for r in range(2):
                q = 2 * h + r
                d2d2_copies[q] = send(pbuf.at[q, other], d2d2.at[q], d2d2_sem, (q,), partner)

    sgn = 1 - 2 * core

    def at(k):
        return lax.rem(chip + sgn * k + chips, chips)

    names = ("far", "relay", "relay_back", "next", "back", "two", "two_back")
    slot = {name: i for i, name in enumerate(names)}
    rs2_copies, ag2_copies, fw2_copies = {}, {}, {}

    def rs_send(q, name, z, k):
        rs2_copies[q, name] = send(sbuf.at[q, z], rs2.at[q, slot[name]], rs2_sem, (q, slot[name]), at(k) * 2 + core)

    def rs_first(q):
        d2d2_copies[q].wait_recv()
        for z in range(chips):
            sbuf[q, z] = pbuf[q, core, z] + d2d2[q, z]
        rs_send(q, "far", at(4), 2)
        rs_send(q, "relay", at(3), 1)
        rs_send(q, "relay_back", at(-3), -1)

    def rs_direct(q):
        rs_send(q, "next", at(1), 1)
        rs_send(q, "back", at(-1), -1)

    def rs_second(q):
        rs2_copies[q, "relay_back"].wait_recv()
        sbuf[q, at(-2)] = sbuf[q, at(-2)] + rs2[q, slot["relay_back"]]
        rs_send(q, "two_back", at(-2), -2)
        rs2_copies[q, "relay"].wait_recv()
        rs2_copies[q, "far"].wait_recv()
        sbuf[q, at(2)] = sbuf[q, at(2)] + rs2[q, slot["relay"]] + rs2[q, slot["far"]]
        rs_send(q, "two", at(2), 2)

    def ag_send(q, name, z, k):
        ref = ybuf.at[q, core, z]
        ag2_copies[q, name] = send(ref, ref, ag2_sem, (q, slot[name]), at(k) * 2 + core)

    def ag_first(q):
        h, r = q // 2, q % 2
        total = sbuf[q, chip]
        for name in ("next", "back", "two_back", "two"):
            rs2_copies[q, name].wait_recv()
            total = total + rs2[q, slot[name]]
        x = xmid[pl.ds(r * rhalf, rhalf), pl.ds(pl.multiple_of(h * hw + me * block, block), block)]
        ybuf[q, core, chip] = (x + total).astype(BF16).astype(F32)
        ag_send(q, "two", chip, 2)
        ag_send(q, "two_back", chip, -2)
        ag_send(q, "next", chip, 1)
        ag_send(q, "back", chip, -1)
        forward2(q, 0, chip)

    def forward2(q, i, z):
        ref = ybuf.at[q, core, z]
        fw2_copies[q, i] = send(ref, ref, fw2_sem, (q, i), partner)

    def ag_second(q):
        ag2_copies[q, "two"].wait_recv()
        ag_send(q, "far", at(-2), 2)
        ag_send(q, "relay", at(-2), 1)
        ag2_copies[q, "two_back"].wait_recv()
        ag_send(q, "relay_back", at(2), -1)
        forward2(q, 1, at(-2))
        forward2(q, 2, at(2))
        ag2_copies[q, "next"].wait_recv()
        forward2(q, 3, at(-1))
        ag2_copies[q, "back"].wait_recv()
        forward2(q, 4, at(1))

    def ag_third(q):
        ag2_copies[q, "relay"].wait_recv()
        forward2(q, 5, at(-3))
        ag2_copies[q, "relay_back"].wait_recv()
        forward2(q, 6, at(3))
        ag2_copies[q, "far"].wait_recv()
        forward2(q, 7, at(4))

    for g in range(GROUPS):
        with scope("attend"):
            for copy in kv_copies[g]:
                copy.wait()

            @pl.loop(0, nb // 4)
            def _(i):
                for j in range(4):
                    attend(g * nb + i * 4 + j)

        if g == 0:
            with scope("barrier"):
                pl.semaphore_wait(barrier, chips)
        start_d2d1(g)
        if g > 0:
            with scope("start_rs1"):
                start_rs1(g - 1)
    with scope("start_rs1"):
        start_rs1(GROUPS - 1)
    for g in range(GROUPS):
        with scope("start_ag1"):
            start_ag1(g)
    with scope("weights_wait"):
        wo_copy.wait()
        for copy in moe_copies:
            copy.wait()
    for g in range(GROUPS):
        with scope("forward1"):
            forward1(g)
    with scope("wait_fw1"):
        for g in range(GROUPS):
            for d in range(chips):
                fw1_copies[g, d].wait_recv()
    with scope("project"):
        project()
    with scope("experts"):
        expert_parts()
    for stage in (rs_first, rs_direct, rs_second, ag_first, ag_second, ag_third):
        for q in range(CHUNKS):
            with scope(stage.__name__):
                stage(q)
    with scope("wait_fw2"):
        for q in range(CHUNKS):
            for i in range(chips):
                fw2_copies[q, i].wait_recv()
    with scope("output"):
        for h in range(2):
            for j in range(group):
                cols = pl.ds(h * hw + j * block, block)
                y = jnp.concatenate([ybuf[2 * h + r, j % 2, j // 2] for r in range(2)], axis=0).astype(BF16)
                for s in range(steps):
                    hidden[s, :, cols] = y[s * batch:(s + 1) * batch]
    with scope("wait_sends"):
        for copy in sends:
            copy.wait_send()


def finish_kernel(y, k, v, hidden, tail_k, tail_v):
    batch, steps, kv_heads, _ = tail_k.shape
    rows = batch * steps
    hidden[...] = y[...]
    for src, dst in ((k, tail_k), (v, tail_v)):
        for b in range(batch):
            for s in range(steps):
                dst[b, s] = src[pl.ds(s * batch + b, kv_heads, stride=rows)].astype(BF16)


def solution(mesh):
    group = mesh.shape["kv"]
    chips = group // 2

    def layer_steps(x_first, next_emb, k_cache, v_cache, seq_len, ln1_gain, ln1_bias, w_q, b_q, w_k, b_k, w_v, b_v, w_o, b_o, ln2_gain, ln2_bias, w_router, w_gate, w_up, w_down, long_factor, expert_idx, route_mask):
        batch, shard_len, kv_heads, head_dim = k_cache.shape
        width = x_first.shape[1]
        steps = next_emb.shape[0] + 1
        q_heads = w_q.shape[1] // head_dim
        experts, _, ff_local = w_gate.shape
        ff = experts * ff_local
        rows = steps * batch
        half = q_heads * steps // 2
        keys = shard_len * kv_heads
        nb = batch // GROUPS
        spc = nb // chips
        rhalf = rows // 2
        block = width // group // 2
        kstep = width // K_CHUNKS
        exponent = np.arange(head_dim // 2, dtype=np.float64) * 2.0 / head_dim
        powers = np.tile((ROPE_BASE ** exponent).astype(np.float32), 2)[None]

        row = lambda vec: vec.reshape(1, -1)
        flat = lambda arr: arr.reshape(batch, keys, head_dim)
        operands = (
            x_first, next_emb, flat(k_cache), flat(v_cache), seq_len, row(ln1_gain), row(ln1_bias),
            w_q, row(b_q), w_k, row(b_k), w_v, row(b_v), w_o, row(b_o), row(ln2_gain), row(ln2_bias), w_router.T,
            w_gate.transpose(2, 0, 1).reshape(ff, width), w_up.transpose(2, 0, 1).reshape(ff, width),
            w_down.transpose(1, 0, 2).reshape(ff, width), row(long_factor), jnp.asarray(powers),
            expert_idx.transpose(0, 2, 1), route_mask,
        )
        any_spec = pl.BlockSpec(memory_space=pl.ANY)
        in_specs = [any_spec] * len(operands)
        in_specs[4] = pl.BlockSpec(memory_space=pltpu.SMEM)
        vmem = pl.BlockSpec(memory_space=pltpu.VMEM)
        V = pltpu.VMEM
        dma = pltpu.SemaphoreType.DMA
        scratch = [
            V((steps, batch, width), BF16), V((steps, batch, width), BF16),
            V((1, width), F32), V((1, width), F32), V((1, width), F32), V((1, width), F32), V((1, width), F32),
            V((1, q_heads * head_dim), F32), V((1, kv_heads * head_dim), F32), V((1, kv_heads * head_dim), F32),
            V((1, head_dim // 2), F32), V((1, head_dim), F32), V((experts, width), BF16),
            V((steps, expert_idx.shape[2], batch), jnp.int32), V(route_mask.shape, jnp.int32),
            V((K_CHUNKS, kstep, q_heads * head_dim), BF16),
            V((K_CHUNKS, kstep, kv_heads * head_dim), BF16), V((K_CHUNKS, kstep, kv_heads * head_dim), BF16),
            V((batch, keys, head_dim), BF16), V((batch, keys, head_dim), BF16), V(w_o.shape, BF16),
            V((rows, q_heads * head_dim), F32), V((rows, kv_heads * head_dim), F32), V((rows, kv_heads * head_dim), F32),
            V((q_heads * rows, head_dim), F32), V((16 * batch, head_dim), F32), V((16 * batch, head_dim), F32),
            V((2 * half, keys), jnp.int32),
            V((2, batch, half + 8, head_dim), F32), V((batch, half + 8, head_dim), F32), V((batch, half + 8, head_dim), F32),
            V((GROUPS, chips, spc, half + 8, head_dim), F32), V((GROUPS, 2, chips, spc, half, head_dim), F32),
            V((rows, q_heads * head_dim), F32), V((rows, width), F32), V((rows, width), BF16),
            V((CHUNKS, 2, chips, rhalf, block), F32), V((CHUNKS, chips, rhalf, block), F32),
            V((CHUNKS, chips, rhalf, block), F32), V((CHUNKS, 7, rhalf, block), F32), V((CHUNKS, 2, chips, rhalf, block), F32),
            dma((15,)), dma((3, K_CHUNKS)), dma((2, GROUPS)), dma((1,)), dma((3, 2)),
            dma((2, GROUPS)), dma((2, GROUPS, chips)), dma((2, GROUPS, chips)), dma((2, GROUPS, chips)),
            dma((2, CHUNKS)), dma((2, CHUNKS, 7)), dma((2, CHUNKS, 7)), dma((2, CHUNKS, chips)),
        ]
        tail_shape = jax.ShapeDtypeStruct((kv_heads, rows, head_dim), F32)
        out = pl.pallas_call(
            functools.partial(kernel, group),
            out_shape=(jax.ShapeDtypeStruct((steps, batch, width), BF16), tail_shape, tail_shape),
            in_specs=in_specs,
            out_specs=(vmem, vmem, vmem),
            scratch_shapes=scratch,
            name="decode_layer",
            compiler_params=pltpu.CompilerParams(
                collective_id=0, has_side_effects=True, vmem_limit_bytes=66_000_000),
        )(*operands)
        final_tail = jax.ShapeDtypeStruct((batch, steps, kv_heads, head_dim), BF16)
        return pl.pallas_call(
            finish_kernel,
            out_shape=(jax.ShapeDtypeStruct((steps, batch, width), BF16), final_tail, final_tail),
            in_specs=[vmem] * 3,
            out_specs=(vmem,) * 3,
            name="finish",
        )(out[0], out[1].reshape(kv_heads * rows, head_dim), out[2].reshape(kv_heads * rows, head_dim))

    replicated = P()
    in_specs = (P('dp'), P(None, 'dp'), P('dp', 'kv'), P('dp', 'kv'), P('dp')) + (replicated,) * 13 + (P(None, None, 'kv'), P(None, None, 'kv'), P(None, 'kv'), replicated, P(None, 'dp'), P(None, 'dp'))
    out_specs = (P(None, 'dp'), P('dp'), P('dp'))
    return jax.shard_map(layer_steps, mesh=mesh, in_specs=in_specs, out_specs=out_specs, check_vma=False)
```

```python
import contextlib
import functools
import math

import jax
import jax.numpy as jnp
import numpy as np
from jax import lax
from jax.experimental import pallas as pl
from jax.experimental.pallas import tpu as pltpu
from jax.sharding import PartitionSpec as P

ROPE_BASE = 10000.0
ROPE_MSCALE = math.sqrt(1.0 + math.log(32.0) / math.log(4096.0))
NORM_EPS = 1e-5
NEG_FILL = -1e30
MESH = pl.DeviceIdType.MESH
F32 = jnp.float32
BF16 = jnp.bfloat16
GROUPS = 2
CHUNKS = 4
scope = contextlib.nullcontext
K_CHUNKS = 8
DEPTH = 5
TILE = 128


def iota(shape, dim):
    return lax.broadcasted_iota(jnp.int32, shape, dim)


def layer_norm_rows(x_f32, gain, bias):
    inv = 1.0 / x_f32.shape[-1]
    mean = jnp.sum(x_f32, axis=-1, keepdims=True) * inv
    centered = x_f32 - mean
    var = jnp.sum(centered * centered, axis=-1, keepdims=True) * inv
    return (centered * lax.rsqrt(var + NORM_EPS) * gain + bias).astype(BF16)


def dot_nt(a, b):
    return lax.dot_general(a, b, (((1,), (1,)), ((), ())), preferred_element_type=F32)


def dot_nn(a, b):
    return jnp.dot(a, b, preferred_element_type=F32)


def kernel(
    group,
    x_first, next_emb, kc, vc, seq_len, ln1_g, ln1_b, wq, bq, wk, bk, wv, bv, wo, bo, ln2_g, ln2_b, wr,
    wg, wu, wd, long_factor, powers, idx, mask,
    hidden, tail_k, tail_v,
    xbuf, hbuf, ln1g_v, ln1b_v, ln2g_v, ln2b_v, bo_v, bq_v, bk_v, bv_v, lf_v, pw_v, wr_v, idx_v, mask_v,
    wq_v, wk_v, wv_v, kc_v, vc_v, wo_v, wg_v, wu_v, wd_v, acc_q, acc_k, acc_v, q2, k2, v2, tcol, cos_v, sin_v,
    stat, d2d1, rs1_send, rs1, obuf, osum, xmid, h2, pbuf, d2d2, sbuf, rs2, ybuf,
    small_sem, qkv_sem, kv_sem, wo_sem, moe_sem, ex_sem,
    d2d1_sem, rs1_sem, ag1_sem, fw1_sem, d2d2_sem, rs2_sem, ag2_sem, fw2_sem,
):
    batch, width = x_first.shape
    steps = next_emb.shape[0] + 1
    rows = steps * batch
    chips = group // 2
    q_heads = wq.shape[1] // TILE
    kv_heads = wk.shape[1] // TILE
    nb = batch // GROUPS
    spc = nb // chips
    half = q_heads * steps // 2
    qrows = 2 * half
    keys = kc.shape[1]
    shard_len = keys // kv_heads
    kstep = width // K_CHUNKS
    ff = wg.shape[0]
    experts = wr.shape[0]
    block = width // group // 2
    scale = TILE ** -0.5

    me = lax.axis_index("kv")
    chip = lax.div(me, 2)
    core = lax.rem(me, 2)
    partner = me + 1 - 2 * core
    other = 1 - core

    def peer_chip(d):
        return lax.rem(chip + d, chips)

    def peer(d):
        return peer_chip(d) * 2 + core

    order = sorted(range(1, chips), key=lambda d: -min(d, chips - d))
    arrive = sorted(range(1, chips), key=lambda d: min(d, chips - d))

    barrier = pltpu.get_barrier_semaphore()
    smalls = [
        (x_first, xbuf.at[0]), (next_emb, xbuf.at[pl.ds(1, steps - 1)]), (ln1_g, ln1g_v), (ln1_b, ln1b_v),
        (long_factor, lf_v), (powers, pw_v), (bq, bq_v), (bk, bk_v), (bv, bv_v), (bo, bo_v),
        (ln2_g, ln2g_v), (ln2_b, ln2b_v), (wr, wr_v), (idx, idx_v), (mask, mask_v),
    ]
    small_copies = [pltpu.make_async_copy(src, dst, small_sem.at[i]) for i, (src, dst) in enumerate(smalls)]
    for copy in small_copies[:6]:
        copy.start()

    q_cols, k_cols = wq_v.shape[2], wk_v.shape[2]
    q_own = pl.ds(pl.multiple_of(core * q_cols, q_cols), q_cols)
    k_own = pl.ds(pl.multiple_of(core * k_cols, k_cols), k_cols)

    def qkv_copies(k):
        span = pl.ds(pl.multiple_of(k * kstep, kstep), kstep)
        return [
            pltpu.make_async_copy(wq.at[span, q_own], wq_v.at[k], qkv_sem.at[0, k]),
            pltpu.make_async_copy(wk.at[span, k_own], wk_v.at[k], qkv_sem.at[1, k]),
            pltpu.make_async_copy(wv.at[span, k_own], wv_v.at[k], qkv_sem.at[2, k]),
        ]

    for k in range(DEPTH):
        for copy in qkv_copies(k):
            copy.start(priority=1)
    for copy in small_copies[6:]:
        copy.start()
    kv_copies = []
    for g in range(GROUPS):
        span = pl.ds(g * nb, nb)
        kv_copies.append([
            pltpu.make_async_copy(kc.at[span], kc_v.at[span], kv_sem.at[0, g]),
            pltpu.make_async_copy(vc.at[span], vc_v.at[span], kv_sem.at[1, g]),
        ])
    wo_copy = pltpu.make_async_copy(wo, wo_v, wo_sem.at[0])
    moe_copies = [pltpu.make_async_copy(src, dst, moe_sem.at[i]) for i, (src, dst) in enumerate(((wg, wg_v), (wu, wu_v), (wd, wd_v)))]
    hw = width // 2

    pl.semaphore_signal(barrier, inc=1, device_id={"kv": partner}, device_id_type=MESH)
    for d in order:
        pl.semaphore_signal(barrier, inc=1, device_id={"kv": peer(d)}, device_id_type=MESH)

    for copy in small_copies[:6]:
        copy.wait()
    for s in range(steps):
        hbuf[s] = layer_norm_rows(xbuf[s].astype(F32), ln1g_v[...], ln1b_v[...])

    acc_q[...] = jnp.zeros_like(acc_q)
    acc_k[...] = jnp.zeros_like(acc_k)
    acc_v[...] = jnp.zeros_like(acc_v)

    row_k = iota((qrows, keys), 0)
    col_k = iota((qrows, keys), 1)
    head_of_row = (row_k * 43) >> 9
    pos = me * shard_len + (col_k >> 2)
    tcol[...] = jnp.where(head_of_row == (col_k & 3), pos, jnp.int32(1 << 30))
    lane = iota((batch, TILE), 1)
    sub = iota((batch, TILE), 0)
    lens = jnp.zeros((batch, TILE), jnp.int32)
    for b in range(batch):
        lens = jnp.where(sub == b, seq_len[b], lens)
    lf = jnp.concatenate([lf_v[...], lf_v[...]], axis=1)
    inv_freq = 1.0 / (lf * pw_v[...])
    sign = jnp.where(lane < TILE // 2, -1.0, 1.0)
    for s in range(steps):
        angles = (lens + s).astype(F32) * inv_freq
        cos_v[pl.ds(s * batch, batch)] = jnp.cos(angles) * ROPE_MSCALE
        sin_v[pl.ds(s * batch, batch)] = jnp.sin(angles) * ROPE_MSCALE * sign

    @pl.loop(0, K_CHUNKS)
    def _(k):
        for copy in qkv_copies(k):
            copy.wait()

        @pl.when(k + DEPTH < K_CHUNKS)
        def _():
            for copy in qkv_copies(k + DEPTH):
                copy.start(priority=1)

        for g in range(GROUPS):
            @pl.when(k == K_CHUNKS - DEPTH + 2 * g)
            def _():
                for copy in kv_copies[g]:
                    copy.start(priority=1)

        h = hbuf[:, :, pl.ds(pl.multiple_of(k * kstep, kstep), kstep)].reshape(rows, kstep)
        acc_q[...] += dot_nn(h, wq_v[k])
        acc_k[...] += dot_nn(h, wk_v[k])
        acc_v[...] += dot_nn(h, wv_v[k])

    wo_copy.start(priority=1)
    for copy in small_copies[6:]:
        copy.wait()

    sends = []

    def send(src, dst, sems, slot, device):
        copy = pltpu.make_async_remote_copy(
            src_ref=src, dst_ref=dst, send_sem=sems.at[(0,) + slot], recv_sem=sems.at[(1,) + slot],
            device_id={"kv": device}, device_id_type=MESH)
        copy.start()
        sends.append(copy)
        return copy

    def rotate(x):
        x = x.astype(BF16).astype(F32)
        return (x * cos_v[...] + pltpu.roll(x, TILE // 2, 1) * sin_v[...]).astype(BF16).astype(F32)

    q_span = pl.ds(pl.multiple_of(core * (q_heads // 2 * rows), rows), q_heads // 2 * rows)
    k_span = pl.ds(pl.multiple_of(core * (kv_heads // 2 * rows), rows), kv_heads // 2 * rows)

    def head_rows(i, per):
        return pl.ds(pl.multiple_of((core * per + i) * rows, rows), rows)

    def head_cols(i, per):
        return pl.ds(pl.multiple_of((core * per + i) * TILE, TILE), TILE)

    half_q, half_kv = q_heads // 2, kv_heads // 2
    for i in range(half_q):
        q2[head_rows(i, half_q)] = rotate(acc_q[:, pl.ds(i * TILE, TILE)] + bq_v[:, head_cols(i, half_q)])
    with scope("barrier"):
        pl.semaphore_wait(barrier, chips)
    exchanges = [send(q2.at[q_span], q2.at[q_span], ex_sem, (0,), partner)]
    for i in range(half_kv):
        cols = pl.ds(i * TILE, TILE)
        k2[head_rows(i, half_kv)] = rotate(acc_k[:, cols] + bk_v[:, head_cols(i, half_kv)])
        v2[head_rows(i, half_kv)] = (acc_v[:, cols] + bv_v[:, head_cols(i, half_kv)]).astype(BF16).astype(F32)
    exchanges.append(send(k2.at[k_span], k2.at[k_span], ex_sem, (1,), partner))
    exchanges.append(send(v2.at[k_span], v2.at[k_span], ex_sem, (2,), partner))
    pad = pl.ds(kv_heads * rows, k2.shape[0] - kv_heads * rows)
    k2[pad] = jnp.zeros((k2.shape[0] - kv_heads * rows, TILE), F32)
    v2[pad] = jnp.zeros((v2.shape[0] - kv_heads * rows, TILE), F32)

    eye = iota((half, TILE), 0) == iota((half, TILE), 1)
    sub8 = iota((8, TILE), 0)

    def to_row(col):
        return jnp.sum(jnp.where(eye, jnp.broadcast_to(col, (half, TILE)), 0.0), axis=0, keepdims=True)

    def to_col(row):
        return jnp.sum(jnp.where(eye, jnp.broadcast_to(row, (half, TILE)), 0.0), axis=1, keepdims=True)

    def pair_tile(m_row, l_row):
        return jnp.where(sub8 == 0, m_row, jnp.where(sub8 == 1, l_row, 0.0))

    def attend(b):
        q = q2[pl.ds(b, qrows, stride=batch)].astype(BF16)
        scores = dot_nt(q, kc_v[b]) * scale
        keep = tcol[...] < seq_len[b]
        scores = jnp.where(keep, scores, NEG_FILL)
        top = jnp.max(scores, axis=1, keepdims=True)
        w = jnp.where(keep, jnp.exp(scores - top), 0.0)
        total = jnp.sum(w, axis=1, keepdims=True)
        out = dot_nn(w.astype(BF16), vc_v[b])
        for hf in range(2):
            part = slice(hf * half, (hf + 1) * half)
            stat[hf, b, pl.ds(0, half)] = out[part]
            stat[hf, b, pl.ds(half, 8)] = pair_tile(to_row(top[part]), to_row(total[part]))

    d2d1_copies, rs1_copies, ag1_copies, fw1_copies = {}, {}, {}, {}
    d2d2_copies = {}

    def merge_pair(b):
        own, got = stat[core, b], d2d1[b]
        m1, l1 = own[half:half + 1], own[half + 1:half + 2]
        m2, l2 = got[half:half + 1], got[half + 1:half + 2]
        top = jnp.maximum(m1, m2)
        a1, a2 = jnp.exp(m1 - top), jnp.exp(m2 - top)
        rs1_send[b, pl.ds(0, half)] = own[:half] * to_col(a1) + got[:half] * to_col(a2)
        rs1_send[b, pl.ds(half, 8)] = pair_tile(top, l1 * a1 + l2 * a2)

    def start_d2d1(g):
        span = pl.ds(g * nb, nb)
        d2d1_copies[g] = send(stat.at[other, span], d2d1.at[span], d2d1_sem, (g,), partner)

    def start_rs1(g):
        d2d1_copies[g].wait_recv()
        for i in range(nb):
            merge_pair(g * nb + i)
        for d in order:
            span = pl.ds(g * nb + peer_chip(d) * spc, spc)
            rs1_copies[g, d] = send(rs1_send.at[span], rs1.at[g, d], rs1_sem, (g, d), peer(d))

    def tail_stats(b):
        q = q2[pl.ds(b + core * (half * batch), half, stride=batch)].astype(BF16)
        k = k2[pl.ds(b, 16, stride=batch)].astype(BF16)
        v = v2[pl.ds(b, 16, stride=batch)].astype(BF16)
        r, j = iota((half, 16), 0), iota((half, 16), 1)
        r3, j3 = (r * 43) >> 7, (j * 43) >> 7
        head = core * (kv_heads // 2) + (r3 >> 2)
        keep = (j3 == head) & ((j - j3 * steps) <= (r - r3 * steps))
        scores = jnp.where(keep, dot_nt(q, k) * scale, NEG_FILL)
        top = jnp.max(scores, axis=1, keepdims=True)
        w = jnp.where(keep, jnp.exp(scores - top), 0.0)
        total = jnp.sum(w, axis=1, keepdims=True)
        return dot_nn(w.astype(BF16), v), to_row(top), to_row(total)

    def start_ag1(g):
        tails = [tail_stats(g * nb + chip * spc + i) for i in range(spc)]
        for d in arrive:
            rs1_copies[g, d].wait_recv()
        for i in range(spc):
            b = g * nb + chip * spc + i
            own = rs1_send[b]
            units = [tails[i], (own[:half], own[half:half + 1], own[half + 1:half + 2])]
            for d in arrive:
                got = rs1[g, d, i]
                units.append((got[:half], got[half:half + 1], got[half + 1:half + 2]))
            top = functools.reduce(jnp.maximum, [u[1] for u in units])
            o_sum, l_sum = 0.0, 0.0
            for o, m, l in units:
                a = jnp.exp(m - top)
                l_sum = l_sum + l * a
                o_sum = o_sum + o * to_col(a)
            obuf[g, core, chip, i] = o_sum / to_col(l_sum)
        own_ref = obuf.at[g, core, chip]
        for d in order:
            ag1_copies[g, d] = send(own_ref, own_ref, ag1_sem, (g, d), peer(d))
        fw1_copies[g, 0] = send(own_ref, own_ref, fw1_sem, (g, 0), partner)

    def forward1(g):
        for d in arrive:
            ag1_copies[g, d].wait_recv()
            ref = obuf.at[g, core, peer_chip(chips - d)]
            fw1_copies[g, d] = send(ref, ref, fw1_sem, (g, d), partner)

    obuf_rows = obuf.reshape(GROUPS, 2, nb * half, TILE)

    def project():
        for hf in range(2):
            for i in range(q_heads // 2):
                parts = [obuf_rows.at[g, hf][pl.ds(i * steps + s, nb, stride=half)]
                         for s in range(steps) for g in range(GROUPS)]
                col = hf * (q_heads // 2) + i
                osum[:, pl.ds(col * TILE, TILE)] = jnp.concatenate(parts, axis=0)
        o = osum[...].astype(BF16)
        for n in range(2):
            cols = pl.ds(n * hw, hw)
            x = xbuf[:, :, cols].astype(F32).reshape(rows, hw)
            val = x + dot_nn(o, wo_v[:, cols]) + bo_v[:, cols]
            xmid[:, cols] = val.astype(BF16).astype(F32)
        h2[...] = layer_norm_rows(xmid[...], ln2g_v[...], ln2b_v[...])

    def gates():
        logits = dot_nt(h2[...], wr_v[...])
        out = []
        e = iota((batch, experts), 1).astype(F32)
        pick = iota((batch, batch), 1) == iota((batch, batch), 0)
        for s in range(steps):
            r = logits[s * batch:(s + 1) * batch]
            total = jnp.zeros((batch, experts), F32)
            for k in range(idx_v.shape[1]):
                masked = jnp.where(mask_v[s, :, k, :] == 1, r, NEG_FILL)
                p = jnp.exp(masked - jnp.max(masked, axis=1, keepdims=True))
                p = p / jnp.sum(p, axis=1, keepdims=True)
                row = jnp.broadcast_to(idx_v[s, pl.ds(k, 1), :].astype(F32), (batch, batch))
                col = jnp.sum(jnp.where(pick, row, 0.0), axis=1, keepdims=True)
                total = total + jnp.where(col == e, p, 0.0)
            out.append(total)
        gate = jnp.concatenate(out, axis=0)
        gate = jnp.concatenate([gate, jnp.zeros((rows, TILE - experts), F32)], axis=1)
        shift = experts
        while shift < TILE:
            gate = gate + pltpu.roll(gate, shift, 1)
            shift *= 2
        reps = -(-ff // TILE)
        return jnp.concatenate([gate] * reps, axis=1)[:, :ff]

    rhalf = rows // 2

    def expert_parts():
        gate = gates()
        ag = dot_nt(h2[...], wg_v[...])
        au = dot_nt(h2[...], wu_v[...])
        u = (gate * (ag * (1.0 / (1.0 + jnp.exp(-ag)))) * au).astype(BF16)
        for h in range(2):
            part = dot_nn(u, wd_v[:, pl.ds(h * hw, hw)]).astype(BF16).astype(F32)
            for j in range(group):
                for r in range(2):
                    pbuf[2 * h + r, j % 2, j // 2] = part[r * rhalf:(r + 1) * rhalf, j * block:(j + 1) * block]
            for r in range(2):
                q = 2 * h + r
                d2d2_copies[q] = send(pbuf.at[q, other], d2d2.at[q], d2d2_sem, (q,), partner)

    sgn = 1 - 2 * core

    def at(k):
        return lax.rem(chip + sgn * k + chips, chips)

    names = ("far", "relay", "relay_back", "next", "back", "two", "two_back")
    slot = {name: i for i, name in enumerate(names)}
    rs2_copies, ag2_copies, fw2_copies = {}, {}, {}

    def rs_send(q, name, z, k):
        rs2_copies[q, name] = send(sbuf.at[q, z], rs2.at[q, slot[name]], rs2_sem, (q, slot[name]), at(k) * 2 + core)

    def rs_first(q):
        d2d2_copies[q].wait_recv()
        for z in range(chips):
            sbuf[q, z] = pbuf[q, core, z] + d2d2[q, z]
        rs_send(q, "far", at(4), 2)
        rs_send(q, "relay", at(3), 1)
        rs_send(q, "relay_back", at(-3), -1)

    def rs_direct(q):
        rs_send(q, "next", at(1), 1)
        rs_send(q, "back", at(-1), -1)

    def rs_second(q):
        rs2_copies[q, "relay_back"].wait_recv()
        sbuf[q, at(-2)] = sbuf[q, at(-2)] + rs2[q, slot["relay_back"]]
        rs_send(q, "two_back", at(-2), -2)
        rs2_copies[q, "relay"].wait_recv()
        rs2_copies[q, "far"].wait_recv()
        sbuf[q, at(2)] = sbuf[q, at(2)] + rs2[q, slot["relay"]] + rs2[q, slot["far"]]
        rs_send(q, "two", at(2), 2)

    def ag_send(q, name, z, k):
        ref = ybuf.at[q, core, z]
        ag2_copies[q, name] = send(ref, ref, ag2_sem, (q, slot[name]), at(k) * 2 + core)

    def ag_first(q):
        h, r = q // 2, q % 2
        total = sbuf[q, chip]
        for name in ("next", "back", "two_back", "two"):
            rs2_copies[q, name].wait_recv()
            total = total + rs2[q, slot[name]]
        x = xmid[pl.ds(r * rhalf, rhalf), pl.ds(pl.multiple_of(h * hw + me * block, block), block)]
        ybuf[q, core, chip] = (x + total).astype(BF16).astype(F32)
        ag_send(q, "two", chip, 2)
        ag_send(q, "two_back", chip, -2)
        ag_send(q, "next", chip, 1)
        ag_send(q, "back", chip, -1)
        forward2(q, 0, chip)

    def forward2(q, i, z):
        ref = ybuf.at[q, core, z]
        fw2_copies[q, i] = send(ref, ref, fw2_sem, (q, i), partner)

    def ag_second(q):
        ag2_copies[q, "two"].wait_recv()
        ag_send(q, "far", at(-2), 2)
        ag_send(q, "relay", at(-2), 1)
        ag2_copies[q, "two_back"].wait_recv()
        ag_send(q, "relay_back", at(2), -1)
        forward2(q, 1, at(-2))
        forward2(q, 2, at(2))
        ag2_copies[q, "next"].wait_recv()
        forward2(q, 3, at(-1))
        ag2_copies[q, "back"].wait_recv()
        forward2(q, 4, at(1))

    def ag_third(q):
        ag2_copies[q, "relay"].wait_recv()
        forward2(q, 5, at(-3))
        ag2_copies[q, "relay_back"].wait_recv()
        forward2(q, 6, at(3))
        ag2_copies[q, "far"].wait_recv()
        forward2(q, 7, at(4))

    def attend_span(first, count):
        @pl.loop(0, count // 4)
        def _(i):
            for j in range(4):
                attend(first + i * 4 + j)

    with scope("wait_exchange"):
        for copy in exchanges:
            copy.wait_recv()
    for g in range(GROUPS):
        for copy in kv_copies[g]:
            copy.wait()
        if g == 0:
            with scope("attend"):
                attend_span(0, nb)
            for copy in moe_copies:
                copy.start(priority=1)
        else:
            with scope("attend"):
                attend_span(g * nb, nb // 2)
            with scope("start_rs1"):
                start_rs1(g - 1)
            with scope("attend"):
                attend_span(g * nb + nb // 2, nb // 2)
        start_d2d1(g)
    tail_k[...] = k2[pl.ds(0, kv_heads * rows)]
    tail_v[...] = v2[pl.ds(0, kv_heads * rows)]
    with scope("start_rs1"):
        start_rs1(GROUPS - 1)
    for g in range(GROUPS):
        with scope("start_ag1"):
            start_ag1(g)
    with scope("weights_wait"):
        wo_copy.wait()
        for copy in moe_copies:
            copy.wait()
    for g in range(GROUPS):
        with scope("forward1"):
            forward1(g)
    with scope("wait_fw1"):
        for g in range(GROUPS):
            for d in range(chips):
                fw1_copies[g, d].wait_recv()
    with scope("project"):
        project()
    with scope("experts"):
        expert_parts()
    for stage in (rs_first, rs_direct, rs_second, ag_first, ag_second, ag_third):
        for q in range(CHUNKS):
            with scope(stage.__name__):
                stage(q)
    with scope("wait_fw2"):
        for q in range(CHUNKS):
            for i in range(chips):
                fw2_copies[q, i].wait_recv()
    with scope("output"):
        for h in range(2):
            for j in range(group):
                cols = pl.ds(h * hw + j * block, block)
                y = jnp.concatenate([ybuf[2 * h + r, j % 2, j // 2] for r in range(2)], axis=0).astype(BF16)
                for s in range(steps):
                    hidden[s, :, cols] = y[s * batch:(s + 1) * batch]
    with scope("wait_sends"):
        for copy in sends:
            copy.wait_send()


def finish_kernel(y, k, v, hidden, tail_k, tail_v):
    batch, steps, kv_heads, _ = tail_k.shape
    rows = batch * steps
    hidden[...] = y[...]
    for src, dst in ((k, tail_k), (v, tail_v)):
        for b in range(batch):
            for s in range(steps):
                dst[b, s] = src[pl.ds(s * batch + b, kv_heads, stride=rows)].astype(BF16)


def solution(mesh):
    group = mesh.shape["kv"]
    chips = group // 2

    def layer_steps(x_first, next_emb, k_cache, v_cache, seq_len, ln1_gain, ln1_bias, w_q, b_q, w_k, b_k, w_v, b_v, w_o, b_o, ln2_gain, ln2_bias, w_router, w_gate, w_up, w_down, long_factor, expert_idx, route_mask):
        batch, shard_len, kv_heads, head_dim = k_cache.shape
        width = x_first.shape[1]
        steps = next_emb.shape[0] + 1
        q_heads = w_q.shape[1] // head_dim
        experts, _, ff_local = w_gate.shape
        ff = experts * ff_local
        rows = steps * batch
        half = q_heads * steps // 2
        keys = shard_len * kv_heads
        nb = batch // GROUPS
        spc = nb // chips
        rhalf = rows // 2
        block = width // group // 2
        kstep = width // K_CHUNKS
        exponent = np.arange(head_dim // 2, dtype=np.float64) * 2.0 / head_dim
        powers = np.tile((ROPE_BASE ** exponent).astype(np.float32), 2)[None]

        row = lambda vec: vec.reshape(1, -1)
        flat = lambda arr: arr.reshape(batch, keys, head_dim)
        operands = (
            x_first, next_emb, flat(k_cache), flat(v_cache), seq_len, row(ln1_gain), row(ln1_bias),
            w_q, row(b_q), w_k, row(b_k), w_v, row(b_v), w_o, row(b_o), row(ln2_gain), row(ln2_bias), w_router.T,
            w_gate.transpose(2, 0, 1).reshape(ff, width), w_up.transpose(2, 0, 1).reshape(ff, width),
            w_down.transpose(1, 0, 2).reshape(ff, width), row(long_factor), jnp.asarray(powers),
            expert_idx.transpose(0, 2, 1), route_mask,
        )
        any_spec = pl.BlockSpec(memory_space=pl.ANY)
        in_specs = [any_spec] * len(operands)
        in_specs[4] = pl.BlockSpec(memory_space=pltpu.SMEM)
        vmem = pl.BlockSpec(memory_space=pltpu.VMEM)
        V = pltpu.VMEM
        dma = pltpu.SemaphoreType.DMA
        scratch = [
            V((steps, batch, width), BF16), V((steps, batch, width), BF16),
            V((1, width), F32), V((1, width), F32), V((1, width), F32), V((1, width), F32), V((1, width), F32),
            V((1, q_heads * head_dim), F32), V((1, kv_heads * head_dim), F32), V((1, kv_heads * head_dim), F32),
            V((1, head_dim // 2), F32), V((1, head_dim), F32), V((experts, width), BF16),
            V((steps, expert_idx.shape[2], batch), jnp.int32), V(route_mask.shape, jnp.int32),
            V((K_CHUNKS, kstep, q_heads * head_dim // 2), BF16),
            V((K_CHUNKS, kstep, kv_heads * head_dim // 2), BF16), V((K_CHUNKS, kstep, kv_heads * head_dim // 2), BF16),
            V((batch, keys, head_dim), BF16), V((batch, keys, head_dim), BF16), V(w_o.shape, BF16),
            V((ff, width), BF16), V((ff, width), BF16), V((ff, width), BF16),
            V((rows, q_heads * head_dim // 2), F32), V((rows, kv_heads * head_dim // 2), F32), V((rows, kv_heads * head_dim // 2), F32),
            V((q_heads * rows, head_dim), F32), V((16 * batch, head_dim), F32), V((16 * batch, head_dim), F32),
            V((2 * half, keys), jnp.int32), V((rows, head_dim), F32), V((rows, head_dim), F32),
            V((2, batch, half + 8, head_dim), F32), V((batch, half + 8, head_dim), F32), V((batch, half + 8, head_dim), F32),
            V((GROUPS, chips, spc, half + 8, head_dim), F32), V((GROUPS, 2, chips, spc, half, head_dim), F32),
            V((rows, q_heads * head_dim), F32), V((rows, width), F32), V((rows, width), BF16),
            V((CHUNKS, 2, chips, rhalf, block), F32), V((CHUNKS, chips, rhalf, block), F32),
            V((CHUNKS, chips, rhalf, block), F32), V((CHUNKS, 7, rhalf, block), F32), V((CHUNKS, 2, chips, rhalf, block), F32),
            dma((15,)), dma((3, K_CHUNKS)), dma((2, GROUPS)), dma((1,)), dma((3,)), dma((2, 3)),
            dma((2, GROUPS)), dma((2, GROUPS, chips)), dma((2, GROUPS, chips)), dma((2, GROUPS, chips)),
            dma((2, CHUNKS)), dma((2, CHUNKS, 7)), dma((2, CHUNKS, 7)), dma((2, CHUNKS, chips)),
        ]
        tail_shape = jax.ShapeDtypeStruct((kv_heads * rows, head_dim), F32)
        out = pl.pallas_call(
            functools.partial(kernel, group),
            out_shape=(jax.ShapeDtypeStruct((steps, batch, width), BF16), tail_shape, tail_shape),
            in_specs=in_specs,
            out_specs=(vmem, vmem, vmem),
            scratch_shapes=scratch,
            name="decode_layer",
            compiler_params=pltpu.CompilerParams(
                collective_id=0, has_side_effects=True, vmem_limit_bytes=66_000_000),
        )(*operands)
        final_tail = jax.ShapeDtypeStruct((batch, steps, kv_heads, head_dim), BF16)
        return pl.pallas_call(
            finish_kernel,
            out_shape=(jax.ShapeDtypeStruct((steps, batch, width), BF16), final_tail, final_tail),
            in_specs=[vmem] * 3,
            out_specs=(vmem,) * 3,
            name="finish",
        )(*out)

    replicated = P()
    in_specs = (P('dp'), P(None, 'dp'), P('dp', 'kv'), P('dp', 'kv'), P('dp')) + (replicated,) * 13 + (P(None, None, 'kv'), P(None, None, 'kv'), P(None, 'kv'), replicated, P(None, 'dp'), P(None, 'dp'))
    out_specs = (P(None, 'dp'), P('dp'), P('dp'))
    return jax.shard_map(layer_steps, mesh=mesh, in_specs=in_specs, out_specs=out_specs, check_vma=False)
```
